32 devices in a mesh: lon: 8 (over z, y), lat: 4 (over x, core).
Axes of the slice: x: 2, y: 2, z: 4, core: 2. Of those that a mesh axis runs over, the one named last changes fastest.
Arguments:
- inputs: bfloat16 [32, 1024, 512], P('lat', 'lon'), may hold values from -6 to 6
- d_out: bfloat16 [32, 1024, 512], P('lat', 'lon'), may hold values from -6 to 6
- w_qkv: bfloat16 [512, 1536], replicated, may hold values from -0.25 to 0.25
- w_proj: bfloat16 [512, 512], replicated, may hold values from -0.25 to 0.25
- gain: float32 [512], replicated, may hold values from 0.1 to 1.9
- bias_table: float32 [465, 16], replicated, may hold values from -400 to 400
- rel_index: int32 [128, 128], replicated, may hold values from 0 to 464, as said below
- shifts: int32 [4], P('lat'), may hold values from 1 to 15, as said below
Outputs:
- d_inputs: bfloat16 [32, 1024, 512], P('lat', 'lon')
- g_qkv: float32 [512, 1536], P(('lon', 'lat'))
- g_proj: float32 [512, 512], P(('lon', 'lat'))
- g_gain: float32 [512], P(('lon', 'lat'))
- g_table: float32 [465, 16], replicated
The draws below stay inside these ranges and needn't reach their ends.
Inputs may be any that keep to these rules, and one draw needn't show every extreme that they name: `rel_index`: entry (i, j) depends only on the row and column offsets between window positions i and j, and distinct offsets give distinct entries. `shifts`: some band is shifted by 16 - 1.
All inputs are finite; a program needn't handle non-finite values.
Results may differ from the reference program's by a relative error of at most 0.0095.
Values may be sent and summed in bfloat16 or wider, within the bound.
No kernel may reach another device: no remote copies, remote signals or barrier semaphores. Data moves between devices by JAX's collectives and lax.ppermute only.
A program may use at most 128 MiB of HBM per device.

```python
import jax
import jax.numpy as jnp
from jax import lax

C = 512
H = 16
HD = 32
WH = 8
WW = 16
WIN = 128
NREL = 465
LON_DEV = 128
LAT = 32
LON = 1024
TOKENS = 32768
N_LON = 8


def code_order(key):
    return jax.random.permutation(jax.random.fold_in(key, 11), NREL).astype(jnp.int32)


def draw_rel_index(key, part):
    codes = code_order(key)
    positions = jnp.arange(WIN, dtype=jnp.int32)
    row_pos = positions // WW
    col_pos = positions % WW
    offset = (row_pos[:, None] - row_pos[None, :] + WH - 1) * (2 * WW - 1) + (col_pos[:, None] - col_pos[None, :] + WW - 1)
    return codes[offset].astype(jnp.int32)


def draw_bias_table(key, part):
    drawn_draw = jax.random.normal(jax.random.fold_in(key, 23), (NREL, H), jnp.float32)
    return jnp.clip(drawn_draw, -4.0, 4.0)


def draw_shifts(key, part):
    count_rows = LAT // WH
    base_key = jax.random.fold_in(jax.random.fold_in(key, 43), part)
    values = jax.random.randint(jax.random.fold_in(base_key, 1), (count_rows,), 1, WW)
    chosen_row = jax.random.randint(jax.random.fold_in(base_key, 2), (), 0, count_rows)
    return values.at[chosen_row].set(WW - 1).astype(jnp.int32)


def strengthened(values, stream_key, source, target, shards_of, factor):
    owner, partner = [(jnp.arange(values.shape[dim]) // (values.shape[dim] // shards_of)).reshape([-1 if axis == dim else 1 for axis in range(values.ndim)]) for dim in (source, target)]
    chosen = jax.random.permutation(stream_key, shards_of)[partner]
    strong = (owner == chosen) | (owner == (partner + shards_of // 2) % shards_of)
    return jnp.where(strong, factor * values, values)


def levels(rng, extent, pieces, smallest, top_value):
    def one(position, shards_of):
        steps = jax.random.uniform(jax.random.fold_in(jax.random.fold_in(rng, 6), position), (shards_of,), jnp.float32, smallest / len(pieces), top_value / len(pieces))
        return jnp.repeat(jnp.exp(steps), extent[position] // shards_of).reshape((-1,) + (1,) * (len(extent) - position - 1))

    level = one(*pieces[0])
    for cut in pieces[1:]:
        level = level * one(*cut)
    return level


def gaussian(stream_key, extent, deviation, limit, pieces=(), kind=jnp.bfloat16):
    values = deviation * jax.random.normal(stream_key, extent, jnp.float32)
    if pieces:
        values = values * levels(stream_key, extent, pieces, -0.22, 0.18)
    return jnp.clip(values, -limit, limit).astype(kind)


def gaussian_with(rng, shape, deviation, reach, pieces, heavy, held_as=jnp.bfloat16):
    values = deviation * jax.random.normal(rng, shape, jnp.float32)
    if pieces:
        values = values * levels(rng, shape, pieces, -0.22, 0.18)
    return jnp.clip(strengthened(values, jax.random.fold_in(rng, 3), *heavy), -reach, reach).astype(held_as)


def setup_inputs(seed: int = 0) -> dict:
    key_list = jax.random.split(jax.random.key(seed), 9)
    return {
        "inputs": gaussian_with(key_list[0], (LAT, LON, C), 1.0, 6.0, ((0, 4), (1, 8)), (1, 2, 8, 2.0)),
        "d_out": gaussian(key_list[1], (LAT, LON, C), 1.0, 6.0, ((0, 4), (1, 8))),
        "w_qkv": gaussian(key_list[2], (C, 3 * C), C ** -0.5, 0.25),
        "w_proj": gaussian(key_list[3], (C, C), C ** -0.5, 0.25),
        "gain": jnp.clip(1.0 + 0.18 * jax.random.normal(key_list[4], (C,), jnp.float32), 0.1, 1.9),
        "bias_table": draw_bias_table(jax.random.fold_in(key_list[8], 71), 0),
        "rel_index": draw_rel_index(jax.random.fold_in(key_list[8], 71), 0),
        "shifts": draw_shifts(jax.random.fold_in(key_list[8], 71), 0),
    }


EPSILON = 1e-05

def rounded(value):
    return lax.optimization_barrier(value.astype(jnp.bfloat16)).astype(jnp.float32)

def to_windows(slab_field):
    span_count = slab_field.shape[1] // WW
    return slab_field.reshape(WH, span_count, WW, C).transpose(1, 0, 2, 3).reshape(span_count, WIN, C)

def from_windows(blocks, columns):
    span_count = columns // WW
    return blocks.reshape(span_count, WH, WW, C).transpose(1, 0, 2, 3).reshape(WH, columns, C)

def window_backward(inputs, d_out, w_qkv, w_proj, gain, bias_heads):
    number = inputs.shape[0]
    source = inputs.astype(jnp.float32)
    centred = source - lax.optimization_barrier(jnp.mean(source, axis=-1, keepdims=True))
    inv_std = lax.rsqrt(lax.optimization_barrier(jnp.mean(centred * centred, axis=-1, keepdims=True)) + EPSILON)
    normal_x = centred * inv_std
    normed = (normal_x * gain).astype(jnp.bfloat16).reshape(number * WIN, C)
    projected = rounded(jnp.dot(normed, w_qkv, preferred_element_type=jnp.float32))
    projected = projected.reshape(number, WIN, 3, H, HD)
    queries = projected[:, :, 0]
    key_heads = projected[:, :, 1]
    value_heads = projected[:, :, 2]
    factor = HD ** (-0.5)
    scores = jnp.einsum('nihd,njhd->nhij', queries, key_heads) * factor + bias_heads
    summit = lax.optimization_barrier(jnp.max(scores, axis=-1, keepdims=True))
    raised = jnp.exp(scores - summit)
    attention = raised / lax.optimization_barrier(jnp.sum(raised, axis=-1, keepdims=True))
    soft_low = rounded(attention)
    attended = jnp.einsum('nhij,njhd->nihd', soft_low, value_heads).astype(jnp.bfloat16)
    attended = attended.reshape(number * WIN, C)
    grad_rows = d_out.reshape(number * WIN, C)
    d_heads = rounded(jnp.dot(grad_rows, w_proj.T, preferred_element_type=jnp.float32))
    d_heads = d_heads.reshape(number, WIN, H, HD)
    term_proj = jnp.dot(attended.T, grad_rows, preferred_element_type=jnp.float32)
    d_soft = jnp.einsum('nihd,njhd->nhij', d_heads, value_heads)
    d_value = jnp.einsum('nhij,nihd->njhd', soft_low, d_heads)
    d_scores = attention * (d_soft - lax.optimization_barrier(jnp.sum(attention * d_soft, axis=-1, keepdims=True)))
    d_scores_low = rounded(d_scores)
    d_query = jnp.einsum('nhij,njhd->nihd', d_scores_low, key_heads) * factor
    d_key = jnp.einsum('nhij,nihd->njhd', d_scores_low, queries) * factor
    d_projected = jnp.stack([d_query, d_key, d_value], axis=2).astype(jnp.bfloat16)
    d_projected = d_projected.reshape(number * WIN, 3 * C)
    term_qkv = jnp.dot(normed.T, d_projected, preferred_element_type=jnp.float32)
    d_normed = jnp.dot(d_projected, w_qkv.T, preferred_element_type=jnp.float32).reshape(number, WIN, C)
    term_gain = lax.optimization_barrier(jnp.sum(d_normed * normal_x, axis=(0, 1)))
    scaled = d_normed * gain
    d_branch = inv_std * (scaled - lax.optimization_barrier(jnp.mean(scaled, axis=-1, keepdims=True)) - normal_x * lax.optimization_barrier(jnp.mean(scaled * normal_x, axis=-1, keepdims=True)))
    d_inputs = (d_out.astype(jnp.float32) + d_branch).astype(jnp.bfloat16)
    return (d_inputs, term_qkv, term_proj, term_gain, lax.optimization_barrier(jnp.sum(d_scores, axis=0)))

def reference(inputs, d_out, w_qkv, w_proj, gain, bias_table, rel_index, shifts):
    bias_heads = jnp.transpose(bias_table[rel_index], (2, 0, 1))
    band_count = LAT // WH
    per_block = LON_DEV // WW

    def block_step(running, block_pair):
        result = window_backward(block_pair[0], block_pair[1], w_qkv, w_proj, gain, bias_heads)
        summed = (running[0] + result[1], running[1] + result[2], running[2] + result[3], running[3] + result[4])
        return (summed, result[0])

    def row_step(running, band_item):
        input_band, grad_band, band_shift = band_item
        moved_x = jnp.roll(input_band, band_shift, axis=1)
        moved_d = jnp.roll(grad_band, band_shift, axis=1)
        blocks_x = to_windows(moved_x).reshape(N_LON, per_block, WIN, C)
        blocks_d = to_windows(moved_d).reshape(N_LON, per_block, WIN, C)
        running, d_blocks = lax.scan(block_step, running, (blocks_x, blocks_d))
        d_band = from_windows(d_blocks.reshape(N_LON * per_block, WIN, C), LON)
        return (running, jnp.roll(d_band, -band_shift, axis=1))
    start = (jnp.zeros((C, 3 * C), jnp.float32), jnp.zeros((C, C), jnp.float32), jnp.zeros((C,), jnp.float32), jnp.zeros((H, WIN, WIN), jnp.float32))
    running, d_bands = lax.scan(row_step, start, (inputs.reshape(band_count, WH, LON, C), d_out.reshape(band_count, WH, LON, C), shifts))
    d_inputs = d_bands.reshape(LAT, LON, C)
    grad_scale = TOKENS ** (-0.5)
    table_term = jax.ops.segment_sum(running[3].reshape(H, WIN * WIN).T, rel_index.reshape(WIN * WIN), num_segments=NREL)
    g_table = table_term * (TOKENS // WIN) ** (-0.5)
    return (d_inputs, running[0] * grad_scale, running[1] * grad_scale, running[2] * grad_scale, g_table)
```

```python
import math

import jax
import jax.numpy as jnp
from jax import lax
from jax.experimental import pallas as pl
from jax.experimental.pallas import tpu as pltpu
from jax.sharding import PartitionSpec as P

H = 16
HD = 32
WH = 8
WW = 16
WIN = WH * WW
LANES = 128
SLAB = LANES // HD
SPANS = WH + 1
EPSILON = 1e-05
LOG2E = math.log2(math.e)
BF = jnp.bfloat16
F32 = jnp.float32


def dot(left, right):
    return lax.dot_general(left, right, (((1,), (0,)), ((), ())), preferred_element_type=F32)


def dot_nt(left, right):
    return lax.dot_general(left, right, (((1,), (1,)), ((), ())), preferred_element_type=F32)


def split3(value):
    high = value.astype(BF)
    rest = value - high.astype(F32)
    middle = rest.astype(BF)
    low = (rest - middle.astype(F32)).astype(BF)
    return jnp.concatenate([high, middle, low], axis=0)


def joined3(value):
    rows = value.shape[0] // 3
    return (value[:rows] + value[rows : 2 * rows]) + value[2 * rows :]


def odd_lanes(rows):
    lane = lax.broadcasted_iota(jnp.int32, (rows, LANES), 1)
    return (lane // WW) % 2 == 1


def bias_kernel(code_ref, table_ref, hot_ref, bias_ref, span_ref):
    entries, width = hot_ref.shape
    entry = lax.broadcasted_iota(jnp.int32, (entries, width), 0)
    hot = jnp.where(entry == code_ref[...], 1.0, 0.0).astype(BF)
    hot_ref[...] = hot
    spans = joined3(dot(split3(table_ref[...]), hot)) * LOG2E
    span_ref[...] = spans
    odd = odd_lanes(WW)

    for h in range(H):
        for row in range(WH):
            halves = []
            for parity in range(2):
                first = parity - row + WH - 1
                line = span_ref[h : h + 1, first * LANES : (first + 1) * LANES]
                line = jnp.broadcast_to(line, (WW, LANES))
                turn = (LANES - (WW - 1) + WW * parity) % LANES
                halves.append(pltpu.roll(line, turn, 1, stride=1, stride_axis=0))
            bias_ref[h, row * WW : (row + 1) * WW, :] = jnp.where(odd, halves[1], halves[0])


def expand_bias(code, table):
    entries, width = table.shape[1], code.shape[1]
    return pl.pallas_call(
        bias_kernel,
        out_shape=(
            jax.ShapeDtypeStruct((entries, width), BF),
            jax.ShapeDtypeStruct((H, WIN, WIN), F32),
        ),
        scratch_shapes=[pltpu.VMEM((H, width), F32)],
        name="expand_bias",
    )(code, table)


def norm_stats(rows):
    centred = rows - jnp.mean(rows, axis=-1, keepdims=True)
    inv_std = lax.rsqrt(jnp.mean(centred * centred, axis=-1, keepdims=True) + EPSILON)
    return centred * inv_std, inv_std


def pair_rows(first, second):
    both = jnp.concatenate([first, second], axis=1)
    return both.reshape(both.shape[0] * both.shape[1], both.shape[2])


def shift_matrix(offset):
    row = lax.broadcasted_iota(jnp.int32, (WIN, 2 * WIN), 0)
    col = lax.broadcasted_iota(jnp.int32, (WIN, 2 * WIN), 1)
    same = (row // WW) == (col // (2 * WW))
    hit = same & ((col % (2 * WW)) == (row % WW) + offset)
    return jnp.where(hit, 1.0, 0.0).astype(BF)


def project_kernel(
    shift_ref, xprev_ref, xcur_ref, dprev_ref, dcur_ref, wq_ref, wp_ref, gain_ref, *rest
):
    x_ref, d_ref, nt_ref, qkv_ref, dh_ref, wpt_ref = rest[-6:]

    @pl.when(pl.program_id(0) == 0)
    def _():
        wpt_ref[...] = wp_ref[...].T

    select = shift_matrix(WW - shift_ref[0])
    rows = dot(select, pair_rows(xprev_ref[...], xcur_ref[...]))
    x_ref[0] = rows.astype(BF)
    normal, _ = norm_stats(rows)
    normed = (normal * gain_ref[...]).astype(BF)
    nt_ref[...] = normed.T
    qkv_ref[0] = dot(normed, wq_ref[...]).astype(BF)
    grads = dot(select, pair_rows(dprev_ref[...], dcur_ref[...])).astype(BF)
    d_ref[0] = grads
    dh_ref[0] = dot(grads, wpt_ref[...]).astype(BF)


def project(shift, x, d, w_qkv, w_proj, gain, halo=None, carried=None):
    c = x.shape[-1]
    count = x.shape[1] // WW
    block = (WH, WW, c)
    if carried is None:
        base, steps = 1, count - 1
        prev_x, prev_d = x, d
        more, alias = (), {}
    else:
        base, steps = 0, 1
        prev_x, prev_d = halo
        more, alias = carried, {8 + n: n for n in range(5)}
    full = pl.BlockSpec(memory_space=pl.ANY)
    return pl.pallas_call(
        project_kernel,
        grid=(steps,),
        in_specs=[
            pl.BlockSpec(memory_space=pltpu.SMEM),
            pl.BlockSpec(block, lambda w: (0, w, 0)),
            pl.BlockSpec(block, lambda w: (0, w + base, 0)),
            pl.BlockSpec(block, lambda w: (0, w, 0)),
            pl.BlockSpec(block, lambda w: (0, w + base, 0)),
            pl.BlockSpec(w_qkv.shape, lambda w: (0, 0)),
            pl.BlockSpec(w_proj.shape, lambda w: (0, 0)),
            pl.BlockSpec(gain.shape, lambda w: (0, 0)),
        ]
        + [full for _ in more],
        out_specs=[
            pl.BlockSpec((1, WIN, c), lambda w: (w + base, 0, 0)),
            pl.BlockSpec((1, WIN, c), lambda w: (w + base, 0, 0)),
            pl.BlockSpec((c, WIN), lambda w: (0, w + base)),
            pl.BlockSpec((1, WIN, 3 * c), lambda w: (w + base, 0, 0)),
            pl.BlockSpec((1, WIN, c), lambda w: (w + base, 0, 0)),
        ],
        out_shape=[
            jax.ShapeDtypeStruct((count, WIN, c), BF),
            jax.ShapeDtypeStruct((count, WIN, c), BF),
            jax.ShapeDtypeStruct((c, count * WIN), BF),
            jax.ShapeDtypeStruct((count, WIN, 3 * c), BF),
            jax.ShapeDtypeStruct((count, WIN, c), BF),
        ],
        scratch_shapes=[pltpu.VMEM(w_proj.shape, BF)],
        input_output_aliases=alias,
        name="project_rest" if carried is None else "project_rim",
    )(shift, prev_x, x, prev_d, d, w_qkv, w_proj, gain, *more)


def own_blocks(turned):
    rows = []
    for a in range(SLAB):
        part = turned[a * HD : (a + 1) * HD]
        gap = jnp.zeros_like(part)
        rows.append(jnp.concatenate([part if b == a else gap for b in range(SLAB)], axis=1))
    return jnp.concatenate(rows, axis=0)


def own_lanes(slab):
    lane = lax.broadcasted_iota(jnp.int32, slab.shape, 1)
    return jnp.concatenate(
        [jnp.where(lane // HD == a, slab, jnp.zeros_like(slab)) for a in range(SLAB)], axis=0
    )


def attend_slab(q, k, v, dh, bias_ref, sum_ref, first):
    factor = HD ** (-0.5)
    k_turned, v_turned = k.T, v.T
    scores = dot(k, own_blocks(q.T))
    d_soft = dot(v, own_blocks(dh.T))
    soft_all, d_all, att, dq = [], [], [], []
    for a in range(SLAB):
        lanes = slice(a * WIN, (a + 1) * WIN)
        part = slice(a * HD, (a + 1) * HD)
        score = scores[:, lanes] * (factor * LOG2E) + bias_ref[first + a]
        raised = jnp.exp2(score - jnp.max(score, axis=0, keepdims=True))
        attention = raised * (1.0 / jnp.sum(raised, axis=0, keepdims=True))
        soft_low = attention.astype(BF)
        soft = d_soft[:, lanes]
        d_score = attention * (soft - jnp.sum(attention * soft, axis=0, keepdims=True))
        sum_ref[first + a] += d_score
        d_low = d_score.astype(BF)
        soft_all.append(soft_low)
        d_all.append(d_low)
        att.append(dot(v_turned[part], soft_low))
        dq.append(dot(k_turned[part], d_low))
    att = jnp.concatenate(att, axis=0).astype(BF)
    dq = (jnp.concatenate(dq, axis=0) * factor).astype(BF).T
    dk = (dot(jnp.concatenate(d_all, axis=1), own_lanes(q)) * factor).astype(BF)
    dv = dot(jnp.concatenate(soft_all, axis=1), own_lanes(dh)).astype(BF)
    return att, dq, dk, dv


def fold_table(sum_ref, hot_ref, row_ref, heads):
    odd = odd_lanes(WH)
    for h in range(heads):
        sums = [None, None]
        for col in range(WW):
            tile = sum_ref[h, pl.ds(col, WH, stride=WW), :]
            for parity in range(2):
                kept = jnp.where(odd, tile, 0.0) if parity else jnp.where(odd, 0.0, tile)
                moved = pltpu.roll(kept, (WW - 1 - col - WW * parity) % LANES, 1)
                sums[parity] = moved if col == 0 else sums[parity] + moved
        for parity in range(2):
            row_ref[h, parity * WH : (parity + 1) * WH, :] = sums[parity]
    spans = []
    for first in range(SPANS):
        span = None
        for parity in range(2):
            row = parity + WH - 1 - first
            if 0 <= row < WH:
                part = row_ref[:, parity * WH + row, :]
                span = part if span is None else span + part
        spans.append(span)
    return joined3(dot_nt(split3(jnp.concatenate(spans, axis=1)), hot_ref[...]))


def attend_kernel(scales, last, *refs):
    q_ref, k_ref, v_ref, dh_ref, bias_ref, hot_ref, nt_ref, d_ref = refs[:8]
    if last:
        att0_ref = refs[8]
        dp_ref, grad_ref, table_ref = refs[9:12]
    else:
        dp_ref, att_out_ref, grad_ref, table_ref = refs[8:12]
    att_ref, sum_ref, row_ref = refs[12:]
    w = pl.program_id(0)
    heads = bias_ref.shape[0]
    slabs = heads // SLAB
    wide = slabs * LANES

    @pl.when(w == 0)
    def _():
        sum_ref[...] = jnp.zeros_like(sum_ref)

    for s in range(slabs):
        lanes = slice(s * LANES, (s + 1) * LANES)
        att, dq, dk, dv = attend_slab(
            q_ref[0, :, lanes],
            k_ref[0, :, lanes],
            v_ref[0, :, lanes],
            dh_ref[0, :, lanes],
            bias_ref,
            sum_ref,
            s * SLAB,
        )
        att_ref[lanes, pl.ds(pl.multiple_of(w * WIN, WIN), WIN)] = att
        for n, part in enumerate((dq, dk, dv)):
            dp_ref[w, :, n * wide + s * LANES : n * wide + (s + 1) * LANES] = part

    @pl.when(w == pl.num_programs(0) - 1)
    def _():
        grad_scale, table_scale = scales
        count = dp_ref.shape[0]
        tokens = count * WIN
        c = nt_ref.shape[0]
        grad = dot(nt_ref[...], dp_ref[...].reshape(tokens, 3 * wide))
        grad_ref[:, : 3 * wide] = (grad * grad_scale).astype(BF)
        if last:
            d_rows = d_ref[...].reshape(tokens, c)
            grad = dot(att0_ref[...], d_rows)
            grad_ref[: c - wide, 3 * wide :] = (grad * grad_scale).astype(BF)
            grad = dot(att_ref[...], d_rows)
            grad_ref[c - wide :, 3 * wide :] = (grad * grad_scale).astype(BF)
        else:
            att_out_ref[...] = att_ref[...]
        table_ref[...] = fold_table(sum_ref, hot_ref, row_ref, heads) * table_scale


def attend(group, groups, qkv, dh, bias, hot, nt, d, scales, att0=None):
    count, _, c = dh.shape
    heads = H // groups
    wide = heads * HD
    tokens = count * WIN
    last = att0 is not None
    entries = hot.shape[0]

    def lane_block(n):
        return pl.BlockSpec((1, WIN, wide), lambda w: (w, 0, n))

    def whole(array):
        return pl.BlockSpec(array.shape, lambda w: (0,) * array.ndim)

    columns = 3 * wide + (c if last else 0)
    outs = [jax.ShapeDtypeStruct((count, WIN, 3 * wide), BF)]
    if not last:
        outs.append(jax.ShapeDtypeStruct((wide, tokens), BF))
    outs.append(jax.ShapeDtypeStruct((c, columns), BF))
    outs.append(jax.ShapeDtypeStruct((heads, entries), F32))
    args = [qkv, qkv, qkv, dh, bias, hot, nt, d] + ([att0] if last else [])
    return pl.pallas_call(
        lambda *refs: attend_kernel(scales, last, *refs),
        grid=(count,),
        in_specs=[
            lane_block(group),
            lane_block(groups + group),
            lane_block(2 * groups + group),
            lane_block(group),
            pl.BlockSpec((heads, WIN, WIN), lambda w: (group, 0, 0)),
            whole(hot),
            whole(nt),
            whole(d),
        ]
        + ([whole(att0)] if last else []),
        out_specs=[whole(o) for o in outs],
        out_shape=outs,
        scratch_shapes=[
            pltpu.VMEM((wide, tokens), BF),
            pltpu.VMEM((heads, WIN, WIN), F32),
            pltpu.VMEM((heads, 2 * WH, LANES), F32),
        ],
        name=f"attend_{group}",
    )(*args)


def input_kernel(groups, *refs):
    dp_refs = refs[:groups]
    x_ref, d_ref, w_ref, gain_ref, out_ref, wt_ref = refs[groups:]
    c = x_ref.shape[-1]

    @pl.when(pl.program_id(0) == 0)
    def _():
        wt_ref[...] = w_ref[...].T

    wide = dp_refs[0].shape[-1] // 3
    d_normed = None
    for n in range(3):
        for g in range(groups):
            part = dot(
                dp_refs[g][0, :, n * wide : (n + 1) * wide],
                wt_ref[n * c + g * wide : n * c + (g + 1) * wide, :],
            )
            d_normed = part if d_normed is None else d_normed + part
    normal, inv_std = norm_stats(x_ref[0].astype(F32))
    scaled = d_normed * gain_ref[...]
    branch = inv_std * (
        scaled
        - jnp.mean(scaled, axis=-1, keepdims=True)
        - normal * jnp.mean(scaled * normal, axis=-1, keepdims=True)
    )
    out_ref[0] = (d_ref[0].astype(F32) + branch).astype(BF)


def input_grad(dps, x, d, w_qkv, gain):
    count, _, c = x.shape
    groups = len(dps)
    return pl.pallas_call(
        lambda *refs: input_kernel(groups, *refs),
        grid=(count,),
        in_specs=[pl.BlockSpec((1, WIN, dp.shape[-1]), lambda w: (w, 0, 0)) for dp in dps]
        + [
            pl.BlockSpec((1, WIN, c), lambda w: (w, 0, 0)),
            pl.BlockSpec((1, WIN, c), lambda w: (w, 0, 0)),
            pl.BlockSpec(w_qkv.shape, lambda w: (0, 0)),
            pl.BlockSpec(gain.shape, lambda w: (0, 0)),
        ],
        out_specs=pl.BlockSpec((1, WIN, c), lambda w: (w, 0, 0)),
        out_shape=jax.ShapeDtypeStruct((count, WIN, c), BF),
        scratch_shapes=[pltpu.VMEM(w_qkv.shape[::-1], BF)],
        name="input_grad",
    )(*dps, x, d, w_qkv, gain)


def place_kernel(shift_ref, cur_ref, next_ref, rim_ref, out_ref):
    w = pl.program_id(0)
    final = w == pl.num_programs(0) - 1
    cur = cur_ref[0].reshape(WH, WW, cur_ref.shape[-1])
    after = jnp.where(final, rim_ref[0], next_ref[0]).reshape(WH, WW, cur_ref.shape[-1])
    moved = dot(shift_matrix(shift_ref[0]), pair_rows(cur, after)).astype(BF)
    out_ref[...] = moved.reshape(WH, WW, cur_ref.shape[-1])


def place(shift, windows, rim):
    count, _, c = windows.shape
    return pl.pallas_call(
        place_kernel,
        grid=(count,),
        in_specs=[
            pl.BlockSpec(memory_space=pltpu.SMEM),
            pl.BlockSpec((1, WIN, c), lambda w: (w, 0, 0)),
            pl.BlockSpec((1, WIN, c), lambda w: (jnp.minimum(w + 1, count - 1), 0, 0)),
            pl.BlockSpec((1, WIN, c), lambda w: (0, 0, 0)),
        ],
        out_specs=pl.BlockSpec((WH, WW, c), lambda w: (0, w, 0)),
        out_shape=jax.ShapeDtypeStruct((WH, count * WW, c), BF),
        name="place",
    )(shift, windows, windows, rim)


def flat_permute(value, mask):
    total = lax.axis_size("lon") * lax.axis_size("lat")
    return lax.ppermute(value, ("lon", "lat"), [(n, n ^ mask) for n in range(total)])


def bit_groups(total):
    bits = total.bit_length() - 1
    sizes = [1]
    while sum(sizes) < bits:
        sizes.append(min(2, bits - sum(sizes)))
    return sizes


def scatter_sum(matrix):
    n_lat = lax.axis_size("lat")
    total = lax.axis_size("lon") * n_lat
    me = lax.axis_index("lon") * n_lat + lax.axis_index("lat")
    rows, cols = matrix.shape
    blocks = matrix.reshape(total, rows // total, cols)
    low = 0
    sizes = bit_groups(total)
    for size in sizes:
        ways = 1 << size
        mine = (me >> low) & (ways - 1)
        view = blocks.reshape(blocks.shape[0] // ways, ways, rows // total, cols)
        kept = lax.dynamic_index_in_dim(view, mine, 1, keepdims=False).astype(F32)
        for n in range(1, ways):
            sent = lax.dynamic_index_in_dim(view, mine ^ n, 1, keepdims=False)
            kept = kept + flat_permute(sent, n << low).astype(F32)
        low += size
        blocks = kept if low == sum(sizes) else kept.astype(BF)
    return blocks.reshape(rows // total, cols)


def full_sum(value):
    total = lax.axis_size("lon") * lax.axis_size("lat")
    low = 0
    for size in bit_groups(total):
        parts = [flat_permute(value, n << low) for n in range(1, 1 << size)]
        for part in parts:
            value = value + part
        low += size
    return value


def ring_shift(value, steps):
    count = lax.axis_size("lon")
    return lax.ppermute(value, "lon", [(n, (n + steps) % count) for n in range(count)])


def span_codes(rel_index):
    rel = rel_index.reshape(WH, WW, WH, WW)
    upper = jnp.concatenate([rel[0, 0, ::-1, ::-1], rel[0, 1:, ::-1, 0].T], axis=1)
    lower = jnp.concatenate([rel[1:, 0, 0, ::-1], rel[1:, 1:, 0, 0]], axis=1)
    grid = jnp.concatenate([upper, lower], axis=0)
    grid = jnp.pad(grid, ((0, 0), (0, 1)), constant_values=-1)
    slots = WH // 2
    lines = [grid[n : n + 2 * slots - 1 : 2].reshape(1, slots * 2 * WW) for n in range(SPANS)]
    return jnp.concatenate(lines, axis=1)


def shards(inputs, d_out, w_qkv, w_proj, gain, bias_table, rel_index, shifts):
    n_lon = lax.axis_size("lon")
    n_lat = lax.axis_size("lat")
    n_dev = n_lon * n_lat
    _, columns, c = inputs.shape
    tokens = inputs.shape[0] * columns * n_dev
    scales = (tokens ** (-0.5), (tokens // WIN) ** (-0.5))
    groups = 2
    gain_row = gain.reshape(1, c)

    rim = (inputs[:, columns - WW :], d_out[:, columns - WW :])
    halo = (ring_shift(rim[0], 1), ring_shift(rim[1], 1))

    relations, _ = bias_table.shape
    entries = -(-relations // LANES) * LANES
    table = jnp.pad(bias_table.T, ((0, 0), (0, entries - relations)))
    hot, bias = expand_bias(span_codes(rel_index), table)

    carried = project(shifts, inputs, d_out, w_qkv, w_proj, gain_row)
    x, d, nt, qkv, dh = project(
        shifts, inputs, d_out, w_qkv, w_proj, gain_row, halo=halo, carried=tuple(carried)
    )

    dp0, att0, grad0, table0 = attend(0, groups, qkv, dh, bias, hot, nt, d, scales)
    own0 = scatter_sum(grad0)
    dp1, grad1, table1 = attend(1, groups, qkv, dh, bias, hot, nt, d, scales, att0=att0)
    own1 = scatter_sum(grad1)

    windows = input_grad((dp0, dp1), x, d, w_qkv, gain_row)
    returned = ring_shift(windows[:1], -1)
    d_inputs = place(shifts, windows, returned)

    g_table = full_sum(jnp.concatenate([table0, table1], axis=0))[:, :relations].T

    wide = c // groups
    parts = []
    for n in range(3):
        parts += [own0[:, n * wide : (n + 1) * wide], own1[:, n * wide : (n + 1) * wide]]
    g_qkv = jnp.concatenate(parts, axis=1)
    g_proj = own1[:, 3 * wide :]
    rows = c // n_dev
    start = (lax.axis_index("lon") * n_lat + lax.axis_index("lat")) * rows
    w_rows = lax.dynamic_slice_in_dim(w_qkv, start, rows, 0).astype(F32)
    gain_rows = lax.dynamic_slice_in_dim(gain, start, rows, 0)
    g_gain = jnp.sum(w_rows * g_qkv, axis=1) / gain_rows
    return (d_inputs, g_qkv, g_proj, g_gain, g_table)


def solution(mesh):
    return jax.shard_map(
        shards,
        mesh=mesh,
        in_specs=(P("lat", "lon", None), P("lat", "lon", None), P(), P(), P(), P(), P(), P("lat")),
        out_specs=(
            P("lat", "lon", None),
            P(("lon", "lat"), None),
            P(("lon", "lat"), None),
            P(("lon", "lat")),
            P(),
        ),
        check_vma=False,
    )
```

```python
import math

import jax
import jax.numpy as jnp
from jax import lax
from jax.experimental import pallas as pl
from jax.experimental.pallas import tpu as pltpu
from jax.sharding import PartitionSpec as P


H = 16
HD = 32
WH = 8
WW = 16
WIN = WH * WW
LANES = 128
SLAB = LANES // HD
SPANS = WH + 1
UNIT = 16
EPSILON = 1e-05
LOG2E = math.log2(math.e)
BF = jnp.bfloat16
F32 = jnp.float32
PARAMS = pltpu.CompilerParams(vmem_limit_bytes=24 * 2**20)


def dot(left, right):
    return lax.dot_general(left, right, (((1,), (0,)), ((), ())), preferred_element_type=F32)


def dot_nt(left, right):
    return lax.dot_general(left, right, (((1,), (1,)), ((), ())), preferred_element_type=F32)


def split3(value):
    high = value.astype(BF)
    rest = value - high.astype(F32)
    middle = rest.astype(BF)
    low = (rest - middle.astype(F32)).astype(BF)
    return jnp.concatenate([high, middle, low], axis=0)


def joined3(value):
    rows = value.shape[0] // 3
    return (value[:rows] + value[rows : 2 * rows]) + value[2 * rows :]


def bits_of(me_ref, low, size):
    return lax.shift_right_logical(me_ref[0], low) & ((1 << size) - 1)


def odd_lanes(rows):
    lane = lax.broadcasted_iota(jnp.int32, (rows, LANES), 1)
    return (lane // WW) % 2 == 1


def bias_kernel(me_ref, rel_ref, table_ref, hot_ref, bias_ref, line_ref, span_ref):
    line_ref[...] = rel_ref[...].astype(F32).T
    slot = lax.broadcasted_iota(jnp.int32, (1, LANES), 1) % (2 * WW)
    codes = []
    for first in range(SPANS):
        row = max(WH - 1 - first, 0)
        parity = first + row - (WH - 1)
        near = line_ref[row * WW + WW - 1 : row * WW + WW, :]
        far = line_ref[row * WW : row * WW + 1, :]
        if parity:
            near = pltpu.roll(near, LANES - WW, 1)
        far = pltpu.roll(far, (WW - 1 - WW * parity) % LANES, 1)
        code = jnp.where(slot < WW, near, far)
        codes.append(jnp.where(slot == 2 * WW - 1, -1.0, code))
    code = jnp.concatenate(codes, axis=1).astype(jnp.int32)
    entry = lax.broadcasted_iota(jnp.int32, hot_ref.shape, 0)
    hot = jnp.where(entry == code, 1.0, 0.0).astype(BF)
    hot_ref[...] = hot
    span_ref[...] = joined3(dot(split3(table_ref[...]), hot)) * LOG2E
    odd = odd_lanes(WW)
    for h in range(H):
        for row in range(WH):
            halves = []
            for parity in range(2):
                first = parity - row + WH - 1
                line = span_ref[h : h + 1, first * LANES : (first + 1) * LANES]
                line = jnp.broadcast_to(line, (WW, LANES))
                turn = (LANES - (WW - 1) + WW * parity) % LANES
                halves.append(pltpu.roll(line, turn, 1, stride=1, stride_axis=0))
            bias_ref[h, row * WW : (row + 1) * WW, :] = jnp.where(odd, halves[1], halves[0])


def expand_bias(me, rel_index, table):
    width = SPANS * LANES
    whole = pl.BlockSpec(memory_space=pltpu.VMEM)
    return pl.pallas_call(
        bias_kernel,
        in_specs=[pl.BlockSpec(memory_space=pltpu.SMEM), whole, whole],
        out_shape=(
            jax.ShapeDtypeStruct((table.shape[1], width), BF),
            jax.ShapeDtypeStruct((H, WIN, WIN), F32),
        ),
        scratch_shapes=[pltpu.VMEM((WIN, WIN), F32), pltpu.VMEM((H, width), F32)],
        compiler_params=PARAMS,
        name="expand_bias",
    )(me, rel_index, table)


def norm_stats(rows):
    centred = rows - jnp.mean(rows, axis=-1, keepdims=True)
    inv_std = lax.rsqrt(jnp.mean(centred * centred, axis=-1, keepdims=True) + EPSILON)
    return centred * inv_std, inv_std


def pair_rows(first, second):
    both = jnp.concatenate([first, second], axis=1)
    return both.reshape(both.shape[0] * both.shape[1], both.shape[2])


def shift_matrix(offset):
    row = lax.broadcasted_iota(jnp.int32, (WIN, 2 * WIN), 0)
    col = lax.broadcasted_iota(jnp.int32, (WIN, 2 * WIN), 1)
    same = (row // WW) == (col // (2 * WW))
    hit = same & ((col % (2 * WW)) == (row % WW) + offset)
    return jnp.where(hit, 1.0, 0.0).astype(BF)


def project_kernel(
    shift_ref, rim_ref, x_ref, d_ref, wq_ref, wp_ref, gain_ref, *rest
):
    xw_ref, dw_ref, nt_ref, qkv_ref, dh_ref, norm_ref = rest[-6:]
    rim = rim_ref is not None
    count = 1 if rim else x_ref.shape[1] // WW - 1
    c = x_ref.shape[-1]
    tokens = count * WIN
    select = shift_matrix(WW - shift_ref[0])

    def spans(ref, n, halo):
        if rim:
            return pair_rows(rim_ref[halo], ref[...])
        return pair_rows(ref[:, n * WW : (n + 1) * WW, :], ref[:, (n + 1) * WW : (n + 2) * WW, :])

    first = 0 if rim else 1
    for n in range(count):
        rows = slice(n * WIN, (n + 1) * WIN)
        values = dot(select, spans(x_ref, n, 0))
        xw_ref[first + n] = values.astype(BF)
        normal, _ = norm_stats(values)
        normed = (normal * gain_ref[...]).astype(BF)
        norm_ref[rows, :] = normed
        nt_ref[:, (first + n) * WIN : (first + n + 1) * WIN] = normed.T
        dw_ref[first + n] = dot(select, spans(d_ref, n, 1)).astype(BF)
    step = 2 * LANES
    for n in range(3 * c // step):
        cols = slice(n * step, (n + 1) * step)
        part = dot(norm_ref[...], wq_ref[:, cols]).astype(BF)
        qkv_ref[first:, :, cols] = part.reshape(count, WIN, step)
    grads = dw_ref[first:].reshape(tokens, c)
    for n in range(c // step):
        cols = slice(n * step, (n + 1) * step)
        part = dot_nt(grads, wp_ref[cols, :]).astype(BF)
        dh_ref[first:, :, cols] = part.reshape(count, WIN, step)


def project(shift, x, d, w_qkv, w_proj, gain, halo=None, carried=None):
    c = x.shape[-1]
    count = x.shape[1] // WW
    outs = [
        jax.ShapeDtypeStruct((count, WIN, c), BF),
        jax.ShapeDtypeStruct((count, WIN, c), BF),
        jax.ShapeDtypeStruct((c, count * WIN), BF),
        jax.ShapeDtypeStruct((count, WIN, 3 * c), BF),
        jax.ShapeDtypeStruct((count, WIN, c), BF),
    ]
    scalar = pl.BlockSpec(memory_space=pltpu.SMEM)
    if carried is None:
        whole = pl.BlockSpec(memory_space=pltpu.VMEM)
        return pl.pallas_call(
            lambda shift_ref, *refs: project_kernel(shift_ref, None, *refs),
            in_specs=[scalar] + [whole] * 5,
            out_shape=outs,
            scratch_shapes=[pltpu.VMEM(((count - 1) * WIN, c), BF)],
            compiler_params=PARAMS,
            name="project_rest",
        )(shift, x, d, w_qkv, w_proj, gain)
    block = pl.BlockSpec((WH, WW, c), lambda w: (0, 0, 0))

    def one(array):
        return pl.BlockSpec(array.shape, lambda w: (0,) * array.ndim)

    return pl.pallas_call(
        project_kernel,
        grid=(1,),
        in_specs=[scalar, one(halo), block, block, one(w_qkv), one(w_proj), one(gain)]
        + [pl.BlockSpec(memory_space=pl.ANY) for _ in carried],
        out_specs=[
            pl.BlockSpec((1, WIN, c), lambda w: (0, 0, 0)),
            pl.BlockSpec((1, WIN, c), lambda w: (0, 0, 0)),
            pl.BlockSpec((c, WIN), lambda w: (0, 0)),
            pl.BlockSpec((1, WIN, 3 * c), lambda w: (0, 0, 0)),
            pl.BlockSpec((1, WIN, c), lambda w: (0, 0, 0)),
        ],
        out_shape=outs,
        scratch_shapes=[pltpu.VMEM((WIN, c), BF)],
        input_output_aliases={7 + n: n for n in range(5)},
        compiler_params=PARAMS,
        name="project_rim",
    )(shift, halo, x, d, w_qkv, w_proj, gain, *carried)


def own_blocks(turned):
    rows = []
    for a in range(SLAB):
        part = turned[a * HD : (a + 1) * HD]
        gap = jnp.zeros_like(part)
        rows.append(jnp.concatenate([part if b == a else gap for b in range(SLAB)], axis=1))
    return jnp.concatenate(rows, axis=0)


def own_lanes(slab):
    lane = lax.broadcasted_iota(jnp.int32, slab.shape, 1)
    return jnp.concatenate(
        [jnp.where(lane // HD == a, slab, jnp.zeros_like(slab)) for a in range(SLAB)], axis=0
    )


def attend_slab(q, k, v, dh, bias_ref, sum_ref, head, first):
    factor = HD ** (-0.5)
    k_turned, v_turned = k.T, v.T
    scores = dot(k, own_blocks(q.T))
    d_soft = dot(v, own_blocks(dh.T))
    soft_all, d_all, att, dq = [], [], [], []
    for a in range(SLAB):
        lanes = slice(a * WIN, (a + 1) * WIN)
        part = slice(a * HD, (a + 1) * HD)
        score = scores[:, lanes] * (factor * LOG2E) + bias_ref[head + first + a]
        raised = jnp.exp2(score - jnp.max(score, axis=0, keepdims=True))
        attention = raised * (1.0 / jnp.sum(raised, axis=0, keepdims=True))
        soft_low = attention.astype(BF)
        soft = d_soft[:, lanes]
        d_score = attention * (soft - jnp.sum(attention * soft, axis=0, keepdims=True))
        sum_ref[first + a] += d_score
        d_low = d_score.astype(BF)
        soft_all.append(soft_low)
        d_all.append(d_low)
        att.append(dot(v_turned[part], soft_low))
        dq.append(dot(k_turned[part], d_low))
    att = jnp.concatenate(att, axis=0).astype(BF)
    dq = (jnp.concatenate(dq, axis=0) * factor).astype(BF).T
    dk = (dot(jnp.concatenate(d_all, axis=1), own_lanes(q)) * factor).astype(BF)
    dv = dot(jnp.concatenate(soft_all, axis=1), own_lanes(dh)).astype(BF)
    return att, dq, dk, dv


def fold_table(sum_ref, hot_ref, row_ref, heads):
    odd = odd_lanes(WH)
    for h in range(heads):
        sums = [None, None]
        for col in range(WW):
            tile = sum_ref[h, pl.ds(col, WH, stride=WW), :]
            for parity in range(2):
                kept = jnp.where(odd, tile, 0.0) if parity else jnp.where(odd, 0.0, tile)
                moved = pltpu.roll(kept, (WW - 1 - col - WW * parity) % LANES, 1)
                sums[parity] = moved if col == 0 else sums[parity] + moved
        for parity in range(2):
            row_ref[h, parity * WH : (parity + 1) * WH, :] = sums[parity]
    spans = []
    for first in range(SPANS):
        span = None
        for parity in range(2):
            row = parity + WH - 1 - first
            if 0 <= row < WH:
                part = row_ref[:, parity * WH + row, :]
                span = part if span is None else span + part
        spans.append(span)
    return joined3(dot_nt(split3(jnp.concatenate(spans, axis=1)), hot_ref[...]))


def attend_kernel(scales, slabs, base, split, *refs):
    core_ref, qkv_ref, dh_ref, bias_ref, hot_ref, nt_ref, d_ref = refs[:7]
    dp_ref, att_ref, sum_ref, row_ref = refs[7], refs[-3], refs[-2], refs[-1]
    count, _, c = dh_ref.shape
    heads = slabs * SLAB
    wide = slabs * LANES
    tokens = count * WIN
    sum_ref[...] = jnp.zeros_like(sum_ref)

    def window(w, carry):
        for s in range(slabs):
            at = (base + s) * LANES
            att, dq, dk, dv = attend_slab(
                qkv_ref[w, :, at : at + LANES],
                qkv_ref[w, :, c + at : c + at + LANES],
                qkv_ref[w, :, 2 * c + at : 2 * c + at + LANES],
                dh_ref[w, :, at : at + LANES],
                bias_ref,
                sum_ref,
                base * SLAB,
                s * SLAB,
            )
            lanes = slice(s * LANES, (s + 1) * LANES)
            att_ref[lanes, pl.ds(pl.multiple_of(w * WIN, WIN), WIN)] = att
            for n, part in enumerate((dq, dk, dv)):
                dp_ref[w, :, n * wide + s * LANES : n * wide + (s + 1) * LANES] = part
        return carry

    lax.fori_loop(0, count, window, 0)
    grad_scale, table_scale = scales
    table = fold_table(sum_ref, hot_ref, row_ref, heads) * table_scale
    d_rows = d_ref[...].reshape(tokens, c)
    if not split:
        grad_ref, proj_ref, table_ref = refs[8:11]
        for n in range(3 * slabs):
            cols = slice(n * LANES, (n + 1) * LANES)
            part = dp_ref[:, :, cols].reshape(tokens, LANES)
            grad_ref[:, cols] = (dot(nt_ref[...], part) * grad_scale).astype(BF)
        proj_ref[...] = (dot(att_ref[...], d_rows) * grad_scale).astype(BF)
        table_ref[...] = table
        return
    kept_ref, sent_ref, table_ref, both_ref = refs[8:12]
    core = bits_of(core_ref, 0, 1)
    low = 2 * kept_ref.shape[0]
    top = c // (low * UNIT)
    per_top = 3 * slabs
    for n in range(0, per_top, 2):
        wide_n = min(2, per_top - n)
        part = dp_ref[:, :, n * LANES : (n + wide_n) * LANES].reshape(tokens, wide_n * LANES)
        grad = (dot(nt_ref[...], part) * grad_scale).astype(BF)
        for t in range(top):
            for b in range(low):
                row = (t * low + b) * UNIT
                for m in range(wide_n):
                    both_ref[(b % 2) ^ core, b // 2, t * per_top + n + m] = grad[
                        row : row + UNIT, m * LANES : (m + 1) * LANES
                    ]
    tiles = c // LANES
    grad = (dot(att_ref[...], d_rows) * grad_scale).astype(BF)
    for s in range(slabs):
        for b in range(low):
            row = (s * low + b) * UNIT
            for m in range(tiles):
                both_ref[(b % 2) ^ core, b // 2, top * per_top + s * tiles + m] = grad[
                    row : row + UNIT, m * LANES : (m + 1) * LANES
                ]
    table_ref[...] = jnp.zeros_like(table_ref)
    rows = slice(base * SLAB, base * SLAB + heads)
    entries = table.shape[1]
    for n in range(table_ref.shape[0]):
        lanes = min(LANES, entries - n * LANES)
        table_ref[n, rows, :lanes] = table[:, n * LANES : n * LANES + lanes]
    kept_ref[...] = both_ref[0]
    units = kept_ref.shape[0] * kept_ref.shape[1]
    sent_ref[:units] = both_ref[1].reshape(units, UNIT, LANES)
    sent_ref[units:] = table_ref[...].astype(BF)


def attend(base, slabs, qkv, dh, bias, hot, nt, d, scales, core, n_dev):
    count, _, c = dh.shape
    heads = slabs * SLAB
    wide = heads * HD
    tokens = count * WIN
    entries = hot.shape[0]
    split = c // n_dev == UNIT
    outs = [jax.ShapeDtypeStruct((count, WIN, 3 * wide), BF)]
    scratch = []
    if split:
        top = c // LANES
        low = n_dev // top
        units = top * 3 * slabs + slabs * (c // LANES)
        tables = -(-entries // LANES)
        outs += [
            jax.ShapeDtypeStruct((low // 2, units, UNIT, LANES), BF),
            jax.ShapeDtypeStruct((low // 2 * units + tables, UNIT, LANES), BF),
            jax.ShapeDtypeStruct((tables, UNIT, LANES), F32),
        ]
        scratch = [pltpu.VMEM((2, low // 2, units, UNIT, LANES), BF)]
    else:
        outs += [
            jax.ShapeDtypeStruct((c, 3 * wide), BF),
            jax.ShapeDtypeStruct((wide, c), BF),
            jax.ShapeDtypeStruct((heads, entries), F32),
        ]
    whole = pl.BlockSpec(memory_space=pltpu.VMEM)
    return pl.pallas_call(
        lambda *refs: attend_kernel(scales, slabs, base, split, *refs),
        in_specs=[pl.BlockSpec(memory_space=pltpu.SMEM)] + [whole] * 6,
        out_shape=outs,
        scratch_shapes=scratch
        + [
            pltpu.VMEM((wide, tokens), BF),
            pltpu.VMEM((heads, WIN, WIN), F32),
            pltpu.VMEM((heads, 2 * WH, LANES), F32),
        ],
        compiler_params=PARAMS,
    )(core, qkv, dh, bias, hot, nt, d)


def input_rows(dp_refs, windows, x_ref, d_ref, w_ref, gain_ref, store):
    c = x_ref.shape[-1]
    start, stop = windows
    d_normed = None
    for n in range(3):
        parts = []
        for dp_ref in dp_refs:
            wide = dp_ref.shape[-1] // 3
            part = dp_ref[start:stop, :, n * wide : (n + 1) * wide]
            parts.append(part.reshape((stop - start) * WIN, wide))
        part = dot_nt(jnp.concatenate(parts, axis=1), w_ref[:, n * c : (n + 1) * c])
        d_normed = part if d_normed is None else d_normed + part
    for w in range(start, stop):
        grad = d_normed[(w - start) * WIN : (w - start + 1) * WIN]
        normal, inv_std = norm_stats(x_ref[w].astype(F32))
        scaled = grad * gain_ref[...]
        branch = inv_std * (
            scaled
            - jnp.mean(scaled, axis=-1, keepdims=True)
            - normal * jnp.mean(scaled * normal, axis=-1, keepdims=True)
        )
        store(w, (d_ref[w].astype(F32) + branch).astype(BF))


def input_rim_kernel(dp0_ref, dp1_ref, x_ref, d_ref, w_ref, gain_ref, out_ref):
    def store(w, value):
        out_ref[...] = value

    input_rows((dp0_ref, dp1_ref), (0, 1), x_ref, d_ref, w_ref, gain_ref, store)


def placed(select, first, second):
    c = first.shape[-1]
    pair = pair_rows(first.reshape(WH, WW, c), second.reshape(WH, WW, c))
    return dot(select, pair).astype(BF).reshape(WH, WW, c)


def input_rest_kernel(
    shift_ref, dp0_ref, dp1_ref, x_ref, d_ref, w_ref, gain_ref, rim_ref, out_ref, end_ref, row_ref
):
    count = x_ref.shape[0]
    select = shift_matrix(shift_ref[0])
    row_ref[0] = rim_ref[...]

    def store(w, value):
        row_ref[w] = value

    half = (count + 1) // 2
    for windows in ((1, half), (half, count)):
        input_rows((dp0_ref, dp1_ref), windows, x_ref, d_ref, w_ref, gain_ref, store)
        for w in range(windows[0], windows[1]):
            out_ref[:, (w - 1) * WW : w * WW, :] = placed(select, row_ref[w - 1], row_ref[w])
    end_ref[...] = row_ref[count - 1]


def place_kernel(shift_ref, end_ref, rim_ref, grid_ref, out_ref):
    out_ref[...] = placed(shift_matrix(shift_ref[0]), end_ref[...], rim_ref[...])


def input_rim(dps, x, d, w_qkv, gain):
    return pl.pallas_call(
        input_rim_kernel,
        out_shape=jax.ShapeDtypeStruct(x.shape[1:], BF),
        compiler_params=PARAMS,
        name="input_rim",
    )(*dps, x, d, w_qkv, gain)


def input_rest(shift, dps, x, d, w_qkv, gain, rim):
    count, _, c = x.shape
    whole = pl.BlockSpec(memory_space=pltpu.VMEM)
    return pl.pallas_call(
        input_rest_kernel,
        in_specs=[pl.BlockSpec(memory_space=pltpu.SMEM)] + [whole] * 7,
        out_shape=(
            jax.ShapeDtypeStruct((WH, count * WW, c), BF),
            jax.ShapeDtypeStruct((WIN, c), BF),
        ),
        scratch_shapes=[pltpu.VMEM((count, WIN, c), BF)],
        compiler_params=PARAMS,
        name="input_rest",
    )(shift, *dps, x, d, w_qkv, gain, rim)


def place_last(shift, end, rim, grid):
    last = grid.shape[1] // WW - 1
    c = grid.shape[2]
    one = pl.BlockSpec((WIN, c), lambda n: (0, 0))
    return pl.pallas_call(
        place_kernel,
        grid=(1,),
        in_specs=[
            pl.BlockSpec(memory_space=pltpu.SMEM),
            one,
            one,
            pl.BlockSpec(memory_space=pl.ANY),
        ],
        out_specs=pl.BlockSpec((WH, WW, c), lambda n: (0, last, 0)),
        out_shape=jax.ShapeDtypeStruct(grid.shape, BF),
        input_output_aliases={3: 0},
        compiler_params=PARAMS,
        name="place_last",
    )(shift, end, rim, grid)


def pair_sum(own, parts):
    if len(parts) == 1:
        return own + parts[0]
    return (own + parts[0]) + (parts[1] + parts[2])


def low_kernel(me_ref, kept_ref, got_ref, table_ref, own_ref, sent1_ref, sent2_ref, sent3_ref, out_ref):
    blocks, units = kept_ref.shape[:2]
    table = table_ref[...].astype(BF).astype(F32) + got_ref[blocks * units :].astype(F32)
    out_ref[...] = table
    mine = bits_of(me_ref, 1, 2)
    for n, sent_ref in enumerate((None, sent1_ref, sent2_ref, sent3_ref)):
        b = mine ^ n
        total = kept_ref[b].astype(F32) + got_ref[pl.ds(b * units, units)].astype(F32)
        if n == 0:
            own_ref[...] = total
        else:
            sent_ref[:units] = total.astype(BF)
            sent_ref[units:] = table.astype(BF)


def low_stage(mine, kept, got, table):
    _, units = kept.shape[:2]
    tables = table.shape[0]
    whole = pl.BlockSpec(memory_space=pltpu.VMEM)
    sent = jax.ShapeDtypeStruct((units + tables, UNIT, LANES), BF)
    return pl.pallas_call(
        low_kernel,
        in_specs=[pl.BlockSpec(memory_space=pltpu.SMEM)] + [whole] * 3,
        out_shape=(
            jax.ShapeDtypeStruct((units, UNIT, LANES), F32),
            sent,
            sent,
            sent,
            jax.ShapeDtypeStruct(table.shape, F32),
        ),
        compiler_params=PARAMS,
    )(mine, kept, got, table)


def top_kernel(me_ref, *refs):
    (own0, table0), got0 = refs[:2], refs[2:5]
    (own1, table1), got1 = refs[5:7], refs[7:10]
    own_ref, sent_refs, out_ref, sum0_ref, sum1_ref = refs[10], refs[11:14], refs[14], refs[15], refs[16]
    table = None
    for own, gots, sum_ref, part in ((own0, got0, sum0_ref, table0), (own1, got1, sum1_ref, table1)):
        units = own.shape[0]
        sum_ref[...] = pair_sum(own[...], [g[:units].astype(F32) for g in gots])
        part = pair_sum(part[...].astype(BF).astype(F32), [g[units:].astype(F32) for g in gots])
        table = part if table is None else table + part
    out_ref[...] = table
    top = 1 + len(sent_refs)
    slabs0, slabs1 = (s.shape[0] // (4 * 4) for s in (own0, own1))
    proj0 = own0.shape[0] - slabs0 * 4
    proj1 = own1.shape[0] - slabs1 * 4
    n0, n1 = proj0 // top, proj1 // top
    mine = bits_of(me_ref, 3, 2)
    for n in range(top):
        t = mine ^ n
        target = own_ref if n == 0 else sent_refs[n - 1]
        kind = F32 if n == 0 else BF
        target[:n0] = sum0_ref[pl.ds(t * n0, n0)].astype(kind)
        target[n0 : n0 + n1] = sum1_ref[pl.ds(t * n1, n1)].astype(kind)

        @pl.when(t < slabs0)
        def _():
            target[n0 + n1 : n0 + n1 + 4] = sum0_ref[pl.ds(proj0 + t * 4, 4)].astype(kind)

        @pl.when(t >= slabs0)
        def _():
            target[n0 + n1 : n0 + n1 + 4] = sum1_ref[pl.ds(proj1 + (t - slabs0) * 4, 4)].astype(kind)

        if n:
            target[n0 + n1 + 4 :] = table.astype(BF)


def top_stage(mine, first, second):
    own0, got0, table0 = first
    own1, got1, table1 = second
    tables = table0.shape[0]
    units = (own0.shape[0] + own1.shape[0]) // 4
    whole = pl.BlockSpec(memory_space=pltpu.VMEM)
    sent = jax.ShapeDtypeStruct((units + tables, UNIT, LANES), BF)
    return pl.pallas_call(
        top_kernel,
        in_specs=[pl.BlockSpec(memory_space=pltpu.SMEM)] + [whole] * 10,
        out_shape=(
            jax.ShapeDtypeStruct((units, UNIT, LANES), F32),
            sent,
            sent,
            sent,
            jax.ShapeDtypeStruct(table0.shape, F32),
        ),
        scratch_shapes=[pltpu.VMEM(own0.shape, F32), pltpu.VMEM(own1.shape, F32)],
        compiler_params=PARAMS,
        name="top_stage",
    )(mine, own0, table0, *got0, own1, table1, *got1)


def finish_kernel(
    slabs, me_ref, own_ref, table_ref, got1, got2, got3, w_ref, gain_ref, qkv_ref, proj_ref, g_ref, t_ref
):
    gots = (got1, got2, got3)
    units = own_ref.shape[0]
    total = pair_sum(own_ref[...], [g[:units].astype(F32) for g in gots])
    table = pair_sum(table_ref[...].astype(BF).astype(F32), [g[units:].astype(F32) for g in gots])
    c = proj_ref.shape[1]
    tiles = c // LANES
    unit = 0
    for base, count in ((0, slabs[0]), (slabs[0], slabs[1])):
        for n in range(3):
            for s in range(count):
                at = n * c + (base + s) * LANES
                qkv_ref[:, at : at + LANES] = total[unit]
                unit += 1
    for m in range(tiles):
        proj_ref[:, m * LANES : (m + 1) * LANES] = total[unit + m]
    start = pl.multiple_of(me_ref[0] * UNIT, UNIT)
    rows = w_ref[pl.ds(start, UNIT), :].astype(F32)
    products = jnp.sum(rows * qkv_ref[...], axis=1, keepdims=True)
    lane = lax.broadcasted_iota(jnp.int32, (UNIT, c), 1)
    row = lax.broadcasted_iota(jnp.int32, (UNIT, c), 0)
    gains = jnp.where(lane == start + row, gain_ref[...], 0.0)
    column = products / jnp.sum(gains, axis=1, keepdims=True)
    g_ref[...] = jnp.broadcast_to(column, (UNIT, LANES)).T[:1, :]
    entries = t_ref.shape[1]
    for n in range(table.shape[0]):
        lanes = min(LANES, entries - n * LANES)
        t_ref[:, n * LANES : n * LANES + lanes] = table[n, :, :lanes]


def finish(slabs, me, own, table, gots, w_qkv, gain, entries):
    c = w_qkv.shape[0]
    whole = pl.BlockSpec(memory_space=pltpu.VMEM)
    return pl.pallas_call(
        lambda *refs: finish_kernel(slabs, *refs),
        in_specs=[pl.BlockSpec(memory_space=pltpu.SMEM)] + [whole] * 7,
        out_shape=(
            jax.ShapeDtypeStruct((UNIT, 3 * c), F32),
            jax.ShapeDtypeStruct((UNIT, c), F32),
            jax.ShapeDtypeStruct((1, UNIT), F32),
            jax.ShapeDtypeStruct((H, entries), F32),
        ),
        compiler_params=PARAMS,
        name="finish",
    )(me, own, table, *gots, w_qkv, gain)


def flat_permute(value, mask):
    total = lax.axis_size("lon") * lax.axis_size("lat")
    return lax.ppermute(value, ("lon", "lat"), [(n, n ^ mask) for n in range(total)])


def bit_groups(total):
    bits = total.bit_length() - 1
    sizes = [1]
    while sum(sizes) < bits:
        sizes.append(min(2, bits - sum(sizes)))
    return sizes


def scatter_sum(matrix):
    n_lat = lax.axis_size("lat")
    total = lax.axis_size("lon") * n_lat
    me = lax.axis_index("lon") * n_lat + lax.axis_index("lat")
    rows, cols = matrix.shape
    blocks = matrix.reshape(total, rows // total, cols)
    low = 0
    sizes = bit_groups(total)
    for size in sizes:
        ways = 1 << size
        mine = (me >> low) & (ways - 1)
        view = blocks.reshape(blocks.shape[0] // ways, ways, rows // total, cols)
        kept = lax.dynamic_index_in_dim(view, mine, 1, keepdims=False).astype(F32)
        for n in range(1, ways):
            sent = lax.dynamic_index_in_dim(view, mine ^ n, 1, keepdims=False)
            kept = kept + flat_permute(sent, n << low).astype(F32)
        low += size
        blocks = kept if low == sum(sizes) else kept.astype(BF)
    return blocks.reshape(rows // total, cols)


def full_sum(value):
    total = lax.axis_size("lon") * lax.axis_size("lat")
    low = 0
    for size in bit_groups(total):
        value = pair_sum(value, [flat_permute(value, n << low) for n in range(1, 1 << size)])
        low += size
    return value


def ring_shift(value, steps):
    count = lax.axis_size("lon")
    return lax.ppermute(value, "lon", [(n, (n + steps) % count) for n in range(count)])


def step(inputs, d_out, w_qkv, w_proj, gain, bias_table, rel_index, shifts):
    n_lon = lax.axis_size("lon")
    n_lat = lax.axis_size("lat")
    n_dev = n_lon * n_lat
    _, columns, c = inputs.shape
    tokens = inputs.shape[0] * columns * n_dev
    scales = (tokens ** (-0.5), (tokens // WIN) ** (-0.5))
    entries = bias_table.shape[0]
    gain_row = gain.reshape(1, c)
    me = (lax.axis_index("lon") * n_lat + lax.axis_index("lat")).astype(jnp.int32).reshape(1)
    split = c // n_dev == UNIT and n_lat == 4
    total = c // LANES
    slabs = (total - 1, 1)

    rim = jnp.stack([inputs[:, columns - WW :], d_out[:, columns - WW :]])
    halo = ring_shift(rim, 1)
    hot, bias = expand_bias(me, rel_index, bias_table.T)
    carried = project(shifts, inputs, d_out, w_qkv, w_proj, gain_row)
    x, d, nt, qkv, dh = project(
        shifts, inputs, d_out, w_qkv, w_proj, gain_row, halo=halo, carried=tuple(carried)
    )

    def three(values, low):
        return [flat_permute(value, n << low) for n, value in enumerate(values, 1)]

    shared = (qkv, dh, bias, hot, nt, d, scales, me, n_dev)
    dp0, *out0 = attend(0, slabs[0], *shared)
    if split:
        got0 = flat_permute(out0[1], 1)
    dp1, *out1 = attend(slabs[0], slabs[1], *shared)
    if split:
        got1 = flat_permute(out1[1], 1)
        own0, *sent0, table0 = low_stage(me, out0[0], got0, out0[2])
        got0 = three(sent0, 1)
    first = input_rim((dp0, dp1), x, d, w_qkv, gain_row)
    returned = ring_shift(first, -1)
    if split:
        own1, *sent1, table1 = low_stage(me, out1[0], got1, out1[2])
        got1 = three(sent1, 1)
    grid, end = input_rest(shifts, (dp0, dp1), x, d, w_qkv, gain_row, first)
    if split:
        own, *sent, table = top_stage(me, (own0, got0, table0), (own1, got1, table1))
        got = three(sent, 3)
    d_inputs = place_last(shifts, end, returned, grid)
    if split:
        g_qkv, g_proj, g_gain, g_table = finish(
            slabs, me, own, table, got, w_qkv, gain_row, entries
        )
        return (d_inputs, g_qkv, g_proj, g_gain.reshape(UNIT), g_table.T)

    parts = []
    for n in range(3):
        for out, count in ((out0, slabs[0]), (out1, slabs[1])):
            parts.append(out[0][:, n * count * LANES : (n + 1) * count * LANES])
    parts.append(jnp.concatenate([out0[1], out1[1]], axis=0))
    own = scatter_sum(jnp.concatenate(parts, axis=1))
    g_qkv, g_proj = own[:, : 3 * c], own[:, 3 * c :]
    g_table = full_sum(jnp.concatenate([out0[2], out1[2]], axis=0)).T
    rows = c // n_dev
    w_rows = lax.dynamic_slice_in_dim(w_qkv, me[0] * rows, rows, 0).astype(F32)
    gain_rows = lax.dynamic_slice_in_dim(gain, me[0] * rows, rows, 0)
    g_gain = jnp.sum(w_rows * g_qkv, axis=1) / gain_rows
    return (d_inputs, g_qkv, g_proj, g_gain, g_table)


def solution(mesh):
    return jax.shard_map(
        step,
        mesh=mesh,
        in_specs=(P("lat", "lon", None), P("lat", "lon", None), P(), P(), P(), P(), P(), P("lat")),
        out_specs=(
            P("lat", "lon", None),
            P(("lon", "lat"), None),
            P(("lon", "lat"), None),
            P(("lon", "lat")),
            P(),
        ),
        check_vma=False,
    )
```

```python
import math

import jax
import jax.numpy as jnp
from jax import lax
from jax.experimental import pallas as pl
from jax.experimental.pallas import tpu as pltpu
from jax.sharding import PartitionSpec as P


H = 16
HD = 32
WH = 8
WW = 16
WIN = WH * WW
LANES = 128
SLAB = LANES // HD
SPANS = WH + 1
UNIT = 16
CHAINS = 12
EPSILON = 1e-05
LOG2E = math.log2(math.e)
BF = jnp.bfloat16
F32 = jnp.float32
PARAMS = pltpu.CompilerParams(vmem_limit_bytes=24 * 2**20)
FIRST_PARAMS = pltpu.CompilerParams(vmem_limit_bytes=49 * 2**20)


def dot(left, right):
    return lax.dot_general(left, right, (((1,), (0,)), ((), ())), preferred_element_type=F32)


def dot_nt(left, right):
    return lax.dot_general(left, right, (((1,), (1,)), ((), ())), preferred_element_type=F32)


def split3(value):
    high = value.astype(BF)
    rest = value - high.astype(F32)
    middle = rest.astype(BF)
    low = (rest - middle.astype(F32)).astype(BF)
    return jnp.concatenate([high, middle, low], axis=0)


def joined3(value):
    rows = value.shape[0] // 3
    return (value[:rows] + value[rows : 2 * rows]) + value[2 * rows :]


def device_index():
    return lax.axis_index("lon") * lax.axis_size("lat") + lax.axis_index("lat")


def device_bits(low, size):
    return lax.shift_right_logical(device_index(), low) & ((1 << size) - 1)


def odd_lanes(rows):
    lane = lax.broadcasted_iota(jnp.int32, (rows, LANES), 1)
    return (lane // WW) % 2 == 1


def fill_bias(rel_ref, table_ref, hot_ref, bias_ref, line_ref, span_ref):
    line_ref[...] = rel_ref[...].astype(F32).T
    slot = lax.broadcasted_iota(jnp.int32, (1, LANES), 1) % (2 * WW)
    codes = []
    for first in range(SPANS):
        row = max(WH - 1 - first, 0)
        parity = first + row - (WH - 1)
        near = line_ref[row * WW + WW - 1 : row * WW + WW, :]
        far = line_ref[row * WW : row * WW + 1, :]
        if parity:
            near = pltpu.roll(near, LANES - WW, 1)
        far = pltpu.roll(far, (WW - 1 - WW * parity) % LANES, 1)
        code = jnp.where(slot < WW, near, far)
        codes.append(jnp.where(slot == 2 * WW - 1, -1.0, code))
    code = jnp.concatenate(codes, axis=1).astype(jnp.int32)
    entry = lax.broadcasted_iota(jnp.int32, hot_ref.shape, 0)
    hot = jnp.where(entry == code, 1.0, 0.0).astype(BF)
    hot_ref[...] = hot
    span_ref[...] = joined3(dot(split3(table_ref[...]), hot)) * LOG2E
    odd = odd_lanes(WW)
    for h in range(H):
        for row in range(WH):
            halves = []
            for parity in range(2):
                first = parity - row + WH - 1
                line = span_ref[h : h + 1, first * LANES : (first + 1) * LANES]
                line = jnp.broadcast_to(line, (WW, LANES))
                turn = (LANES - (WW - 1) + WW * parity) % LANES
                halves.append(pltpu.roll(line, turn, 1, stride=1, stride_axis=0))
            bias_ref[h, row * WW : (row + 1) * WW, :] = jnp.where(odd, halves[1], halves[0])


def norm_stats(rows):
    centred = rows - jnp.mean(rows, axis=-1, keepdims=True)
    inv_std = lax.rsqrt(jnp.mean(centred * centred, axis=-1, keepdims=True) + EPSILON)
    return centred * inv_std, inv_std


def pair_rows(first, second):
    both = jnp.concatenate([first, second], axis=1)
    return both.reshape(both.shape[0] * both.shape[1], both.shape[2])


def shift_matrix(offset):
    row = lax.broadcasted_iota(jnp.int32, (WIN, 2 * WIN), 0)
    col = lax.broadcasted_iota(jnp.int32, (WIN, 2 * WIN), 1)
    same = (row // WW) == (col // (2 * WW))
    hit = same & ((col % (2 * WW)) == (row % WW) + offset)
    return jnp.where(hit, 1.0, 0.0).astype(BF)


def project_windows(shift_ref, first, count, spans, wq_ref, wp_ref, gain_ref, outs, norm_ref):
    xw_ref, dw_ref, nt_ref, qkv_ref, dh_ref = outs
    c = wq_ref.shape[0]
    tokens = count * WIN
    select = shift_matrix(WW - shift_ref[0])
    for n in range(count):
        rows = slice(n * WIN, (n + 1) * WIN)
        values = dot(select, spans(0, n))
        xw_ref[first + n] = values.astype(BF)
        normal, _ = norm_stats(values)
        normed = (normal * gain_ref[...]).astype(BF)
        norm_ref[rows, :] = normed
        nt_ref[:, (first + n) * WIN : (first + n + 1) * WIN] = normed.T
    yield
    for n in range(count):
        dw_ref[first + n] = dot(select, spans(1, n)).astype(BF)
    yield
    step = 2 * LANES
    for n in range(3 * c // step):
        cols = slice(n * step, (n + 1) * step)
        part = dot(norm_ref[...], wq_ref[:, cols]).astype(BF)
        qkv_ref[first:, :, cols] = part.reshape(count, WIN, step)
    yield
    grads = dw_ref[first:].reshape(tokens, c)
    for n in range(c // step):
        cols = slice(n * step, (n + 1) * step)
        part = dot_nt(grads, wp_ref[cols, :]).astype(BF)
        dh_ref[first:, :, cols] = part.reshape(count, WIN, step)
    yield


def before_kernel(shift_ref, rel_ref, table_ref, gain_ref, x_hbm, d_hbm, wq_hbm, wp_hbm, *refs):
    outs, (wq_ref, wp_ref, edge_ref, hot_ref, bias_ref) = refs[:5], refs[5:10]
    x_ref, d_ref, norm_ref, line_ref, span_ref, sems = refs[10:]
    pairs = ((x_hbm, x_ref), (d_hbm, d_ref), (wq_hbm, wq_ref), (wp_hbm, wp_ref))
    copies = [
        pltpu.make_async_copy(source, target, sems.at[n])
        for n, (source, target) in enumerate(pairs)
    ]
    for copy in copies:
        copy.start()
    fill_bias(rel_ref, table_ref, hot_ref, bias_ref, line_ref, span_ref)
    count = x_ref.shape[1] // WW - 1

    def spans(which, n):
        ref = (x_ref, d_ref)[which]
        return pair_rows(ref[:, n * WW : (n + 1) * WW, :], ref[:, (n + 1) * WW : (n + 2) * WW, :])

    stages = project_windows(shift_ref, 1, count, spans, wq_ref, wp_ref, gain_ref, outs, norm_ref)
    for copy in copies:
        copy.wait()
        next(stages)
    edge_ref[0] = x_ref[:, :WW, :]
    edge_ref[1] = d_ref[:, :WW, :]


def rim_kernel(shift_ref, halo_ref, edge_ref, wq_ref, wp_ref, gain_ref, *refs):
    def spans(which, n):
        return pair_rows(halo_ref[which], edge_ref[which])

    for _ in project_windows(
        shift_ref, 0, 1, spans, wq_ref, wp_ref, gain_ref, refs[-6:-1], refs[-1]
    ):
        pass


def projected_shapes(count, c):
    return [
        jax.ShapeDtypeStruct((count, WIN, c), BF),
        jax.ShapeDtypeStruct((count, WIN, c), BF),
        jax.ShapeDtypeStruct((c, count * WIN), BF),
        jax.ShapeDtypeStruct((count, WIN, 3 * c), BF),
        jax.ShapeDtypeStruct((count, WIN, c), BF),
    ]


def before(shift, rel_index, table, gain, x, d, w_qkv, w_proj):
    c = x.shape[-1]
    count = x.shape[1] // WW
    scalar = pl.BlockSpec(memory_space=pltpu.SMEM)
    whole = pl.BlockSpec(memory_space=pltpu.VMEM)
    far = pl.BlockSpec(memory_space=pltpu.HBM)
    width = SPANS * LANES
    return pl.pallas_call(
        before_kernel,
        in_specs=[scalar, whole, whole, whole, far, far, far, far],
        out_shape=[pltpu.VMEM(o.shape, o.dtype) for o in projected_shapes(count, c)]
        + [
            pltpu.VMEM(w_qkv.shape, BF),
            pltpu.VMEM(w_proj.shape, BF),
            pltpu.VMEM((2, WH, WW, c), BF),
            pltpu.VMEM((table.shape[1], width), BF),
            pltpu.VMEM((H, WIN, WIN), F32),
        ],
        scratch_shapes=[
            pltpu.VMEM(x.shape, BF),
            pltpu.VMEM(d.shape, BF),
            pltpu.VMEM(((count - 1) * WIN, c), BF),
            pltpu.VMEM((WIN, WIN), F32),
            pltpu.VMEM((H, width), F32),
            pltpu.SemaphoreType.DMA((4,)),
        ],
        compiler_params=FIRST_PARAMS,
        name="before",
    )(shift, rel_index, table, gain, x, d, w_qkv, w_proj)


def project_rim(shift, halo, edge, w_qkv, w_proj, gain, carried):
    count, _, c = carried[0].shape

    def one(array):
        return pl.BlockSpec(array.shape, lambda w: (0,) * array.ndim)

    return pl.pallas_call(
        rim_kernel,
        grid=(1,),
        in_specs=[pl.BlockSpec(memory_space=pltpu.SMEM)]
        + [one(a) for a in (halo, edge, w_qkv, w_proj, gain)]
        + [pl.BlockSpec(memory_space=pl.ANY) for _ in carried],
        out_specs=[
            pl.BlockSpec((1, WIN, c), lambda w: (0, 0, 0)),
            pl.BlockSpec((1, WIN, c), lambda w: (0, 0, 0)),
            pl.BlockSpec((c, WIN), lambda w: (0, 0)),
            pl.BlockSpec((1, WIN, 3 * c), lambda w: (0, 0, 0)),
            pl.BlockSpec((1, WIN, c), lambda w: (0, 0, 0)),
        ],
        out_shape=projected_shapes(count, c),
        scratch_shapes=[pltpu.VMEM((WIN, c), BF)],
        input_output_aliases={6 + n: n for n in range(5)},
        compiler_params=PARAMS,
        name="project_rim",
    )(shift, halo, edge, w_qkv, w_proj, gain, *carried)


def own_blocks(turned):
    rows = []
    for a in range(SLAB):
        part = turned[a * HD : (a + 1) * HD]
        gap = jnp.zeros_like(part)
        rows.append(jnp.concatenate([part if b == a else gap for b in range(SLAB)], axis=1))
    return jnp.concatenate(rows, axis=0)


def own_lanes(slab):
    lane = lax.broadcasted_iota(jnp.int32, slab.shape, 1)
    return jnp.concatenate(
        [jnp.where(lane // HD == a, slab, jnp.zeros_like(slab)) for a in range(SLAB)], axis=0
    )


def attend_scores(q, k, v, dh):
    return dot(k, own_blocks(q.T)), dot(v, own_blocks(dh.T))


def attend_soft(scores, d_soft, bias_ref, sum_ref, head, first):
    factor = HD ** (-0.5)
    soft_all, d_all = [], []
    for a in range(SLAB):
        lanes = slice(a * WIN, (a + 1) * WIN)
        score = scores[:, lanes] * (factor * LOG2E) + bias_ref[head + first + a]
        raised = jnp.exp2(score - jnp.max(score, axis=0, keepdims=True))
        attention = raised * (1.0 / jnp.sum(raised, axis=0, keepdims=True))
        soft_all.append(attention.astype(BF))
        soft = d_soft[:, lanes]
        d_score = attention * (soft - jnp.sum(attention * soft, axis=0, keepdims=True))
        sum_ref[first + a] += d_score
        d_all.append(d_score.astype(BF))
    return soft_all, d_all


def attend_grads(q, k, v, dh, soft_all, d_all):
    factor = HD ** (-0.5)
    k_turned, v_turned = k.T, v.T
    att, dq = [], []
    for a in range(SLAB):
        part = slice(a * HD, (a + 1) * HD)
        att.append(dot(v_turned[part], soft_all[a]))
        dq.append(dot(k_turned[part], d_all[a]))
    att = jnp.concatenate(att, axis=0).astype(BF)
    dq = (jnp.concatenate(dq, axis=0) * factor).astype(BF).T
    dk = (dot(jnp.concatenate(d_all, axis=1), own_lanes(q)) * factor).astype(BF)
    dv = dot(jnp.concatenate(soft_all, axis=1), own_lanes(dh)).astype(BF)
    return att, dq, dk, dv


def fold_table(sum_ref, hot_ref, row_ref, heads):
    odd = odd_lanes(WH)
    for h in range(heads):
        sums = [None, None]
        for col in range(WW):
            tile = sum_ref[h, pl.ds(col, WH, stride=WW), :]
            for parity in range(2):
                kept = jnp.where(odd, tile, 0.0) if parity else jnp.where(odd, 0.0, tile)
                moved = pltpu.roll(kept, (WW - 1 - col - WW * parity) % LANES, 1)
                sums[parity] = moved if col == 0 else sums[parity] + moved
        for parity in range(2):
            row_ref[h, parity * WH : (parity + 1) * WH, :] = sums[parity]
    spans = []
    for first in range(SPANS):
        span = None
        for parity in range(2):
            row = parity + WH - 1 - first
            if 0 <= row < WH:
                part = row_ref[:, parity * WH + row, :]
                span = part if span is None else span + part
        spans.append(span)
    return joined3(dot_nt(split3(jnp.concatenate(spans, axis=1)), hot_ref[...]))


def attend_windows(slabs, base, windows, qkv_ref, dh_ref, bias_ref, sum_ref, dp_ref, att_ref):
    c = dh_ref.shape[-1]
    wide = slabs * LANES
    start, stop = windows
    together = math.gcd(stop - start, max(1, CHAINS // slabs))

    def some(n, carry):
        pieces, operands = [], []
        for m in range(together):
            for s in range(slabs):
                w = start + n * together + m
                at = (base + s) * LANES
                pieces.append((w, s))
                operands.append(
                    [qkv_ref[w, :, i * c + at : i * c + at + LANES] for i in range(3)]
                    + [dh_ref[w, :, at : at + LANES]]
                )
        scores = [attend_scores(*o) for o in operands]
        softs = [
            attend_soft(*scores[i], bias_ref, sum_ref, base * SLAB, s * SLAB)
            for i, (_, s) in enumerate(pieces)
        ]
        for i, (w, s) in enumerate(pieces):
            att, dq, dk, dv = attend_grads(*operands[i], *softs[i])
            lanes = slice(s * LANES, (s + 1) * LANES)
            att_ref[lanes, pl.ds(pl.multiple_of(w * WIN, WIN), WIN)] = att
            for k, part in enumerate((dq, dk, dv)):
                dp_ref[w, :, k * wide + s * LANES : k * wide + (s + 1) * LANES] = part
        return carry

    lax.fori_loop(0, (stop - start) // together, some, 0)


def attend_first_kernel(slabs, base, windows, qkv_ref, dh_ref, bias_ref, dp_ref, att_ref, sum_ref):
    sum_ref[...] = jnp.zeros_like(sum_ref)
    attend_windows(slabs, base, windows, qkv_ref, dh_ref, bias_ref, sum_ref, dp_ref, att_ref)


def attend_kernel(scales, slabs, base, start, split, *refs):
    qkv_ref, dh_ref, bias_ref, hot_ref, nt_ref, d_ref = refs[:6]
    att_ref, sum_ref, row_ref = refs[-3:]
    count, _, c = dh_ref.shape
    heads = slabs * SLAB
    tokens = count * WIN
    if start:
        dp0_ref, att0_ref, sum0_ref = refs[6:9]
        refs = refs[3:]
        sum_ref[...] = sum0_ref[...]
    else:
        sum_ref[...] = jnp.zeros_like(sum_ref)
    dp_ref = refs[6]
    attend_windows(
        slabs, base, (start, count), qkv_ref, dh_ref, bias_ref, sum_ref, dp_ref, att_ref
    )
    if start:
        dp_ref[:start] = dp0_ref[...]
        att_ref[:, : start * WIN] = att0_ref[...]
    grad_scale, table_scale = scales
    table = fold_table(sum_ref, hot_ref, row_ref, heads) * table_scale
    d_rows = d_ref[...].reshape(tokens, c)
    if not split:
        grad_ref, proj_ref, table_ref = refs[7:10]
        for n in range(3 * slabs):
            cols = slice(n * LANES, (n + 1) * LANES)
            part = dp_ref[:, :, cols].reshape(tokens, LANES)
            grad_ref[:, cols] = (dot(nt_ref[...], part) * grad_scale).astype(BF)
        proj_ref[...] = (dot(att_ref[...], d_rows) * grad_scale).astype(BF)
        table_ref[...] = table
        return
    kept_ref, sent_ref, table_ref, both_ref = refs[7:11]
    core = device_bits(0, 1)
    low = 2 * kept_ref.shape[0]
    top = c // (low * UNIT)
    per_top = 3 * slabs
    for n in range(0, per_top, 2):
        wide_n = min(2, per_top - n)
        part = dp_ref[:, :, n * LANES : (n + wide_n) * LANES].reshape(tokens, wide_n * LANES)
        grad = (dot(nt_ref[...], part) * grad_scale).astype(BF)
        for t in range(top):
            for b in range(low):
                row = (t * low + b) * UNIT
                for m in range(wide_n):
                    both_ref[(b % 2) ^ core, b // 2, t * per_top + n + m] = grad[
                        row : row + UNIT, m * LANES : (m + 1) * LANES
                    ]
    tiles = c // LANES
    grad = (dot(att_ref[...], d_rows) * grad_scale).astype(BF)
    for s in range(slabs):
        for b in range(low):
            row = (s * low + b) * UNIT
            for m in range(tiles):
                both_ref[(b % 2) ^ core, b // 2, top * per_top + s * tiles + m] = grad[
                    row : row + UNIT, m * LANES : (m + 1) * LANES
                ]
    table_ref[...] = jnp.zeros_like(table_ref)
    entries = table.shape[1]
    for s in range(slabs):
        for n in range(UNIT // SLAB):
            lanes = min(LANES, entries - n * LANES)
            table_ref[s, n * SLAB : (n + 1) * SLAB, :lanes] = table[
                s * SLAB : (s + 1) * SLAB, n * LANES : n * LANES + lanes
            ]
    kept_ref[...] = both_ref[0]
    units = kept_ref.shape[0] * kept_ref.shape[1]
    sent_ref[:units] = both_ref[1].reshape(units, UNIT, LANES)
    sent_ref[units:] = table_ref[...].astype(BF)


def attend_first(base, slabs, stop, qkv, dh, bias):
    heads = slabs * SLAB
    wide = heads * HD
    return pl.pallas_call(
        lambda *refs: attend_first_kernel(slabs, base, (0, stop), *refs),
        out_shape=(
            jax.ShapeDtypeStruct((stop, WIN, 3 * wide), BF),
            jax.ShapeDtypeStruct((wide, stop * WIN), BF),
            jax.ShapeDtypeStruct((heads, WIN, WIN), F32),
        ),
        compiler_params=PARAMS,
    )(qkv, dh, bias)


def attend(base, slabs, qkv, dh, bias, hot, nt, d, scales, n_dev, split, early=()):
    count, _, c = dh.shape
    heads = slabs * SLAB
    wide = heads * HD
    tokens = count * WIN
    entries = hot.shape[0]
    outs = [jax.ShapeDtypeStruct((count, WIN, 3 * wide), BF)]
    scratch = []
    if split:
        top = c // LANES
        low = n_dev // top
        units = top * 3 * slabs + slabs * (c // LANES)
        outs += [
            jax.ShapeDtypeStruct((low // 2, units, UNIT, LANES), BF),
            jax.ShapeDtypeStruct((low // 2 * units + slabs, UNIT, LANES), BF),
            jax.ShapeDtypeStruct((slabs, UNIT, LANES), F32),
        ]
        scratch = [pltpu.VMEM((2, low // 2, units, UNIT, LANES), BF)]
    else:
        outs += [
            jax.ShapeDtypeStruct((c, 3 * wide), BF),
            jax.ShapeDtypeStruct((wide, c), BF),
            jax.ShapeDtypeStruct((heads, entries), F32),
        ]
    whole = pl.BlockSpec(memory_space=pltpu.VMEM)
    start = early[0].shape[0] if early else 0
    return pl.pallas_call(
        lambda *refs: attend_kernel(scales, slabs, base, start, split, *refs),
        in_specs=[whole] * (6 + len(early)),
        out_shape=outs,
        scratch_shapes=scratch
        + [
            pltpu.VMEM((wide, tokens), BF),
            pltpu.VMEM((heads, WIN, WIN), F32),
            pltpu.VMEM((heads, 2 * WH, LANES), F32),
        ],
        compiler_params=PARAMS,
    )(qkv, dh, bias, hot, nt, d, *early)


def input_rows(dp_refs, windows, x_ref, d_ref, w_ref, gain_ref, store):
    c = x_ref.shape[-1]
    start, stop = windows
    d_normed = None
    for n in range(3):
        parts = []
        for dp_ref in dp_refs:
            wide = dp_ref.shape[-1] // 3
            part = dp_ref[start:stop, :, n * wide : (n + 1) * wide]
            parts.append(part.reshape((stop - start) * WIN, wide))
        part = dot_nt(jnp.concatenate(parts, axis=1), w_ref[:, n * c : (n + 1) * c])
        d_normed = part if d_normed is None else d_normed + part
    for w in range(start, stop):
        grad = d_normed[(w - start) * WIN : (w - start + 1) * WIN]
        normal, inv_std = norm_stats(x_ref[w].astype(F32))
        scaled = grad * gain_ref[...]
        branch = inv_std * (
            scaled
            - jnp.mean(scaled, axis=-1, keepdims=True)
            - normal * jnp.mean(scaled * normal, axis=-1, keepdims=True)
        )
        store(w, (d_ref[w].astype(F32) + branch).astype(BF))


def input_rim_kernel(dp0_ref, dp1_ref, x_ref, d_ref, w_ref, gain_ref, out_ref):
    def store(w, value):
        out_ref[...] = value

    input_rows((dp0_ref, dp1_ref), (0, 1), x_ref, d_ref, w_ref, gain_ref, store)


def placed(select, first, second):
    c = first.shape[-1]
    pair = pair_rows(first.reshape(WH, WW, c), second.reshape(WH, WW, c))
    return dot(select, pair).astype(BF).reshape(WH, WW, c)


def input_rest_kernel(
    shift_ref, dp0_ref, dp1_ref, x_ref, d_ref, w_ref, gain_ref, rim_ref, out_ref, end_ref, row_ref
):
    count = x_ref.shape[0]
    select = shift_matrix(shift_ref[0])
    row_ref[0] = rim_ref[...]

    def store(w, value):
        row_ref[w] = value

    half = (count + 1) // 2
    for windows in ((1, half), (half, count)):
        input_rows((dp0_ref, dp1_ref), windows, x_ref, d_ref, w_ref, gain_ref, store)
        for w in range(windows[0], windows[1]):
            out_ref[:, (w - 1) * WW : w * WW, :] = placed(select, row_ref[w - 1], row_ref[w])
    end_ref[...] = row_ref[count - 1]


def place_kernel(shift_ref, end_ref, rim_ref, grid_ref, out_ref):
    out_ref[...] = placed(shift_matrix(shift_ref[0]), end_ref[...], rim_ref[...])


def input_rim(dps, x, d, w_qkv, gain):
    return pl.pallas_call(
        input_rim_kernel,
        out_shape=jax.ShapeDtypeStruct(x.shape[1:], BF),
        compiler_params=PARAMS,
        name="input_rim",
    )(*dps, x, d, w_qkv, gain)


def input_rest(shift, dps, x, d, w_qkv, gain, rim):
    count, _, c = x.shape
    whole = pl.BlockSpec(memory_space=pltpu.VMEM)
    return pl.pallas_call(
        input_rest_kernel,
        in_specs=[pl.BlockSpec(memory_space=pltpu.SMEM)] + [whole] * 7,
        out_shape=(
            jax.ShapeDtypeStruct((WH, count * WW, c), BF),
            jax.ShapeDtypeStruct((WIN, c), BF),
        ),
        scratch_shapes=[pltpu.VMEM((count, WIN, c), BF)],
        compiler_params=PARAMS,
        name="input_rest",
    )(shift, *dps, x, d, w_qkv, gain, rim)


def place_last(shift, end, rim, grid):
    last = grid.shape[1] // WW - 1
    c = grid.shape[2]
    one = pl.BlockSpec((WIN, c), lambda n: (0, 0))
    return pl.pallas_call(
        place_kernel,
        grid=(1,),
        in_specs=[
            pl.BlockSpec(memory_space=pltpu.SMEM),
            one,
            one,
            pl.BlockSpec(memory_space=pl.ANY),
        ],
        out_specs=pl.BlockSpec((WH, WW, c), lambda n: (0, last, 0)),
        out_shape=jax.ShapeDtypeStruct(grid.shape, BF),
        input_output_aliases={3: 0},
        compiler_params=PARAMS,
        name="place_last",
    )(shift, end, rim, grid)


def pair_sum(own, parts):
    if len(parts) == 1:
        return own + parts[0]
    return (own + parts[0]) + (parts[1] + parts[2])


def low_kernel(kept_ref, got_ref, table_ref, own_ref, sent1_ref, sent2_ref, sent3_ref, out_ref):
    blocks, units = kept_ref.shape[:2]
    table = table_ref[...].astype(BF).astype(F32) + got_ref[blocks * units :].astype(F32)
    out_ref[...] = table
    mine = device_bits(1, 2)
    for n, sent_ref in enumerate((None, sent1_ref, sent2_ref, sent3_ref)):
        b = mine ^ n
        total = kept_ref[b].astype(F32) + got_ref[pl.ds(b * units, units)].astype(F32)
        if n == 0:
            own_ref[...] = total
        else:
            sent_ref[:units] = total.astype(BF)
            sent_ref[units:] = table.astype(BF)


def low_stage(kept, got, table):
    _, units = kept.shape[:2]
    tables = table.shape[0]
    whole = pl.BlockSpec(memory_space=pltpu.VMEM)
    sent = jax.ShapeDtypeStruct((units + tables, UNIT, LANES), BF)
    return pl.pallas_call(
        low_kernel,
        in_specs=[whole] * 3,
        out_shape=(
            jax.ShapeDtypeStruct((units, UNIT, LANES), F32),
            sent,
            sent,
            sent,
            jax.ShapeDtypeStruct(table.shape, F32),
        ),
        compiler_params=PARAMS,
    )(kept, got, table)


def top_kernel(base, slabs, own_ref, table_ref, got1, got2, got3, *refs):
    kept_ref, sent_refs, out_ref, sum_ref = refs[0], refs[1:4], refs[4], refs[5]
    gots = (got1, got2, got3)
    units = own_ref.shape[0]
    sum_ref[...] = pair_sum(own_ref[...], [g[:units].astype(F32) for g in gots])
    table = pair_sum(table_ref[...].astype(BF).astype(F32), [g[units:].astype(F32) for g in gots])
    out_ref[...] = table
    top = 1 + len(sent_refs)
    per_top = 3 * slabs
    tiles = kept_ref.shape[0] - per_top
    mine = device_bits(3, 2)
    for n in range(top):
        t = mine ^ n
        target = kept_ref if n == 0 else sent_refs[n - 1]
        kind = F32 if n == 0 else BF
        target[:per_top] = sum_ref[pl.ds(t * per_top, per_top)].astype(kind)
        here = (t >= base) & (t < base + slabs)
        slab = jnp.clip(t - base, 0, slabs - 1)
        proj = sum_ref[pl.ds(top * per_top + slab * tiles, tiles)]
        target[per_top : per_top + tiles] = jnp.where(here, proj, 0.0).astype(kind)
        if n:
            target[per_top + tiles :] = table.astype(BF)


def top_stage(base, slabs, tiles, own, table, gots):
    units = 3 * slabs + tiles
    whole = pl.BlockSpec(memory_space=pltpu.VMEM)
    sent = jax.ShapeDtypeStruct((units + slabs, UNIT, LANES), BF)
    return pl.pallas_call(
        lambda *refs: top_kernel(base, slabs, *refs),
        in_specs=[whole] * 5,
        out_shape=(
            jax.ShapeDtypeStruct((units, UNIT, LANES), F32),
            sent,
            sent,
            sent,
            jax.ShapeDtypeStruct(table.shape, F32),
        ),
        scratch_shapes=[pltpu.VMEM(own.shape, F32)],
        compiler_params=PARAMS,
    )(own, table, *gots)


def finish_kernel(slabs, *refs):
    w_ref, gain_ref, qkv_ref, proj_ref, g_ref, t_ref = refs[-6:]
    c = proj_ref.shape[1]
    tiles = c // LANES
    entries = t_ref.shape[1]
    base, proj = 0, None
    for group, count in enumerate(slabs):
        own_ref, table_ref, *gots = refs[group * 5 : group * 5 + 5]
        units = own_ref.shape[0]
        total = pair_sum(own_ref[...], [g[:units].astype(F32) for g in gots])
        table = pair_sum(
            table_ref[...].astype(BF).astype(F32), [g[units:].astype(F32) for g in gots]
        )
        for n in range(3):
            for s in range(count):
                at = n * c + (base + s) * LANES
                qkv_ref[:, at : at + LANES] = total[n * count + s]
        part = total[3 * count :]
        proj = part if proj is None else proj + part
        for s in range(count):
            rows = slice((base + s) * SLAB, (base + s + 1) * SLAB)
            for n in range(UNIT // SLAB):
                lanes = min(LANES, entries - n * LANES)
                t_ref[rows, n * LANES : n * LANES + lanes] = table[
                    s, n * SLAB : (n + 1) * SLAB, :lanes
                ]
        base += count
    for m in range(tiles):
        proj_ref[:, m * LANES : (m + 1) * LANES] = proj[m]
    start = pl.multiple_of(device_index() * UNIT, UNIT)
    rows = w_ref[pl.ds(start, UNIT), :].astype(F32)
    products = jnp.sum(rows * qkv_ref[...], axis=1, keepdims=True)
    lane = lax.broadcasted_iota(jnp.int32, (UNIT, c), 1)
    row = lax.broadcasted_iota(jnp.int32, (UNIT, c), 0)
    gains = jnp.where(lane == start + row, gain_ref[...], 0.0)
    column = products / jnp.sum(gains, axis=1, keepdims=True)
    g_ref[...] = jnp.broadcast_to(column, (UNIT, LANES)).T[:1, :]


def finish(slabs, groups, w_qkv, gain, entries):
    c = w_qkv.shape[0]
    whole = pl.BlockSpec(memory_space=pltpu.VMEM)
    args = [a for own, table, gots in groups for a in (own, table, *gots)]
    return pl.pallas_call(
        lambda *refs: finish_kernel(slabs, *refs),
        in_specs=[whole] * (len(args) + 2),
        out_shape=(
            jax.ShapeDtypeStruct((UNIT, 3 * c), F32),
            jax.ShapeDtypeStruct((UNIT, c), F32),
            jax.ShapeDtypeStruct((1, UNIT), F32),
            jax.ShapeDtypeStruct((H, entries), F32),
        ),
        compiler_params=PARAMS,
        name="finish",
    )(*args, w_qkv, gain)


def flat_permute(value, mask):
    total = lax.axis_size("lon") * lax.axis_size("lat")
    return lax.ppermute(value, ("lon", "lat"), [(n, n ^ mask) for n in range(total)])


def bit_groups(total):
    bits = total.bit_length() - 1
    sizes = [1]
    while sum(sizes) < bits:
        sizes.append(min(2, bits - sum(sizes)))
    return sizes


def scatter_sum(matrix):
    n_lat = lax.axis_size("lat")
    total = lax.axis_size("lon") * n_lat
    me = lax.axis_index("lon") * n_lat + lax.axis_index("lat")
    rows, cols = matrix.shape
    blocks = matrix.reshape(total, rows // total, cols)
    low = 0
    sizes = bit_groups(total)
    for size in sizes:
        ways = 1 << size
        mine = (me >> low) & (ways - 1)
        view = blocks.reshape(blocks.shape[0] // ways, ways, rows // total, cols)
        kept = lax.dynamic_index_in_dim(view, mine, 1, keepdims=False).astype(F32)
        for n in range(1, ways):
            sent = lax.dynamic_index_in_dim(view, mine ^ n, 1, keepdims=False)
            kept = kept + flat_permute(sent, n << low).astype(F32)
        low += size
        blocks = kept if low == sum(sizes) else kept.astype(BF)
    return blocks.reshape(rows // total, cols)


def full_sum(value):
    total = lax.axis_size("lon") * lax.axis_size("lat")
    low = 0
    for size in bit_groups(total):
        value = pair_sum(value, [flat_permute(value, n << low) for n in range(1, 1 << size)])
        low += size
    return value


def ring_shift(value, steps):
    count = lax.axis_size("lon")
    return lax.ppermute(value, "lon", [(n, (n + steps) % count) for n in range(count)])


def step(inputs, d_out, w_qkv, w_proj, gain, bias_table, rel_index, shifts):
    n_lon = lax.axis_size("lon")
    n_lat = lax.axis_size("lat")
    n_dev = n_lon * n_lat
    _, columns, c = inputs.shape
    tokens = inputs.shape[0] * columns * n_dev
    scales = (tokens ** (-0.5), (tokens // WIN) ** (-0.5))
    entries = bias_table.shape[0]
    gain_row = gain.reshape(1, c)
    split = c // n_dev == UNIT and n_lat == 4
    total = c // LANES
    slabs = (total - 1, 1)

    rim = jnp.stack([inputs[:, columns - WW :], d_out[:, columns - WW :]])
    halo = ring_shift(rim, 1)
    *carried, w_qkv, w_proj, edge, hot, bias = before(
        shifts, rel_index, bias_table.T, gain_row, inputs, d_out, w_qkv, w_proj
    )
    x, d, nt, qkv, dh = project_rim(shifts, halo, edge, w_qkv, w_proj, gain_row, carried)

    def three(values, low):
        return [flat_permute(value, n << low) for n, value in enumerate(values, 1)]

    tiles = c // LANES
    shared = (qkv, dh, bias, hot, nt, d, scales, n_dev, split)
    dp0, *out0 = attend(0, slabs[0], *shared)
    if split:
        got0 = flat_permute(out0[1], 1)
    early = attend_first(slabs[0], slabs[1], x.shape[0] // 2, qkv, dh, bias)
    if split:
        own0, *sent0, table0 = low_stage(out0[0], got0, out0[2])
        got0 = three(sent0, 1)
    dp1, *out1 = attend(slabs[0], slabs[1], *shared, early=early)
    if split:
        got1 = flat_permute(out1[1], 1)
    first = input_rim((dp0, dp1), x, d, w_qkv, gain_row)
    returned = ring_shift(first, -1)
    if split:
        own1, *sent1, table1 = low_stage(out1[0], got1, out1[2])
        got1 = three(sent1, 1)
        own0, *sent0, table0 = top_stage(0, slabs[0], tiles, own0, table0, got0)
        got0 = three(sent0, 3)
    grid, end = input_rest(shifts, (dp0, dp1), x, d, w_qkv, gain_row, first)
    if split:
        own1, *sent1, table1 = top_stage(slabs[0], slabs[1], tiles, own1, table1, got1)
        got1 = three(sent1, 3)
    d_inputs = place_last(shifts, end, returned, grid)
    if split:
        g_qkv, g_proj, g_gain, g_table = finish(
            slabs, ((own0, table0, got0), (own1, table1, got1)), w_qkv, gain_row, entries
        )
        return (d_inputs, g_qkv, g_proj, g_gain.reshape(UNIT), g_table.T)

    parts = []
    for n in range(3):
        for out, count in ((out0, slabs[0]), (out1, slabs[1])):
            parts.append(out[0][:, n * count * LANES : (n + 1) * count * LANES])
    parts.append(jnp.concatenate([out0[1], out1[1]], axis=0))
    own = scatter_sum(jnp.concatenate(parts, axis=1))
    g_qkv, g_proj = own[:, : 3 * c], own[:, 3 * c :]
    g_table = full_sum(jnp.concatenate([out0[2], out1[2]], axis=0)).T
    rows = c // n_dev
    me = device_index()
    w_rows = lax.dynamic_slice_in_dim(w_qkv, me * rows, rows, 0).astype(F32)
    gain_rows = lax.dynamic_slice_in_dim(gain, me * rows, rows, 0)
    g_gain = jnp.sum(w_rows * g_qkv, axis=1) / gain_rows
    return (d_inputs, g_qkv, g_proj, g_gain, g_table)


def solution(mesh):
    return jax.shard_map(
        step,
        mesh=mesh,
        in_specs=(P("lat", "lon", None), P("lat", "lon", None), P(), P(), P(), P(), P(), P("lat")),
        out_specs=(
            P("lat", "lon", None),
            P(("lon", "lat"), None),
            P(("lon", "lat"), None),
            P(("lon", "lat")),
            P(),
        ),
        check_vma=False,
    )
```

```python
import math

import jax
import jax.numpy as jnp
from jax import lax
from jax.experimental import pallas as pl
from jax.experimental.pallas import tpu as pltpu
from jax.sharding import PartitionSpec as P


H = 16
HD = 32
WH = 8
WW = 16
WIN = WH * WW
LANES = 128
SLAB = LANES // HD
SPANS = WH + 1
UNIT = 16
PIECES = 1
EARLY = 2
CHAINS = 16
EPSILON = 1e-05
LOG2E = math.log2(math.e)
BF = jnp.bfloat16
F32 = jnp.float32
PARAMS = pltpu.CompilerParams(vmem_limit_bytes=24 * 2**20)
FIRST_PARAMS = pltpu.CompilerParams(vmem_limit_bytes=49 * 2**20)


def dot(left, right):
    return lax.dot_general(left, right, (((1,), (0,)), ((), ())), preferred_element_type=F32)


def dot_nt(left, right):
    return lax.dot_general(left, right, (((1,), (1,)), ((), ())), preferred_element_type=F32)


def split3(value):
    high = value.astype(BF)
    rest = value - high.astype(F32)
    middle = rest.astype(BF)
    low = (rest - middle.astype(F32)).astype(BF)
    return jnp.concatenate([high, middle, low], axis=0)


def joined3(value):
    rows = value.shape[0] // 3
    return (value[:rows] + value[rows : 2 * rows]) + value[2 * rows :]


def device_index():
    return lax.axis_index("lon") * lax.axis_size("lat") + lax.axis_index("lat")


def device_bits(low, size):
    return lax.shift_right_logical(device_index(), low) & ((1 << size) - 1)


def odd_lanes(rows):
    lane = lax.broadcasted_iota(jnp.int32, (rows, LANES), 1)
    return (lane // WW) % 2 == 1


def fill_bias(rel_ref, table_ref, hot_ref, bias_ref, line_ref, span_ref):
    line_ref[...] = rel_ref[...].astype(F32).T
    slot = lax.broadcasted_iota(jnp.int32, (1, LANES), 1) % (2 * WW)
    codes = []
    for first in range(SPANS):
        row = max(WH - 1 - first, 0)
        parity = first + row - (WH - 1)
        near = line_ref[row * WW + WW - 1 : row * WW + WW, :]
        far = line_ref[row * WW : row * WW + 1, :]
        if parity:
            near = pltpu.roll(near, LANES - WW, 1)
        far = pltpu.roll(far, (WW - 1 - WW * parity) % LANES, 1)
        code = jnp.where(slot < WW, near, far)
        codes.append(jnp.where(slot == 2 * WW - 1, -1.0, code))
    code = jnp.concatenate(codes, axis=1).astype(jnp.int32)
    entry = lax.broadcasted_iota(jnp.int32, hot_ref.shape, 0)
    hot = jnp.where(entry == code, 1.0, 0.0).astype(BF)
    hot_ref[...] = hot
    span_ref[...] = joined3(dot(split3(table_ref[...]), hot)) * LOG2E
    odd = odd_lanes(WW)
    for h in range(H):
        for row in range(WH):
            halves = []
            for parity in range(2):
                first = parity - row + WH - 1
                line = span_ref[h : h + 1, first * LANES : (first + 1) * LANES]
                line = jnp.broadcast_to(line, (WW, LANES))
                turn = (LANES - (WW - 1) + WW * parity) % LANES
                halves.append(pltpu.roll(line, turn, 1, stride=1, stride_axis=0))
            bias_ref[h, row * WW : (row + 1) * WW, :] = jnp.where(odd, halves[1], halves[0])


def norm_stats(rows):
    centred = rows - jnp.mean(rows, axis=-1, keepdims=True)
    inv_std = lax.rsqrt(jnp.mean(centred * centred, axis=-1, keepdims=True) + EPSILON)
    return centred * inv_std, inv_std


def pair_rows(first, second):
    both = jnp.concatenate([first, second], axis=1)
    return both.reshape(both.shape[0] * both.shape[1], both.shape[2])


def shift_matrix(offset):
    row = lax.broadcasted_iota(jnp.int32, (WIN, 2 * WIN), 0)
    col = lax.broadcasted_iota(jnp.int32, (WIN, 2 * WIN), 1)
    same = (row // WW) == (col // (2 * WW))
    hit = same & ((col % (2 * WW)) == (row % WW) + offset)
    return jnp.where(hit, 1.0, 0.0).astype(BF)


def project_windows(shift_ref, first, count, spans, wq_ref, wp_ref, gain_ref, outs, norm_ref):
    xw_ref, dw_ref, nt_ref, qkv_ref, dh_ref = outs
    c = wq_ref.shape[0]
    tokens = count * WIN
    select = shift_matrix(WW - shift_ref[0])
    for n in range(count):
        rows = slice(n * WIN, (n + 1) * WIN)
        values = dot(select, spans(0, n))
        xw_ref[first + n] = values.astype(BF)
        normal, _ = norm_stats(values)
        normed = (normal * gain_ref[...]).astype(BF)
        norm_ref[rows, :] = normed
        nt_ref[:, (first + n) * WIN : (first + n + 1) * WIN] = normed.T
    yield
    for n in range(count):
        dw_ref[first + n] = dot(select, spans(1, n)).astype(BF)
    yield
    step = 2 * LANES
    for n in range(3 * c // step):
        cols = slice(n * step, (n + 1) * step)
        part = dot(norm_ref[...], wq_ref[:, cols]).astype(BF)
        qkv_ref[first:, :, cols] = part.reshape(count, WIN, step)
    yield
    grads = dw_ref[first:].reshape(tokens, c)
    for n in range(c // step):
        cols = slice(n * step, (n + 1) * step)
        part = dot_nt(grads, wp_ref[cols, :]).astype(BF)
        dh_ref[first:, :, cols] = part.reshape(count, WIN, step)
    yield


def before_kernel(shift_ref, rel_ref, table_ref, gain_ref, x_hbm, d_hbm, wq_hbm, wp_hbm, *refs):
    outs, (wq_ref, wp_ref, edge_ref, last_ref, hot_ref, bias_ref) = refs[:5], refs[5:11]
    x_ref, d_ref, norm_ref, line_ref, span_ref, sems = refs[11:]
    pairs = ((x_hbm, x_ref), (d_hbm, d_ref), (wq_hbm, wq_ref), (wp_hbm, wp_ref))
    copies = []
    for n, (source, target) in enumerate(pairs):
        rows = source.shape[0] // PIECES
        parts = [pl.ds(m * rows, rows) for m in range(PIECES)]
        copies.append(
            [
                pltpu.make_async_copy(source.at[part], target.at[part], sems.at[n, m])
                for m, part in enumerate(parts)
            ]
        )
    for group in copies:
        for copy in group:
            copy.start()
    fill_bias(rel_ref, table_ref, hot_ref, bias_ref, line_ref, span_ref)
    count = x_ref.shape[1] // WW - 1

    def spans(which, n):
        ref = (x_ref, d_ref)[which]
        return pair_rows(ref[:, n * WW : (n + 1) * WW, :], ref[:, (n + 1) * WW : (n + 2) * WW, :])

    stages = project_windows(shift_ref, 1, count, spans, wq_ref, wp_ref, gain_ref, outs, norm_ref)
    for group in copies:
        for copy in group:
            copy.wait()
        next(stages)
    for n, ref in enumerate((x_ref, d_ref)):
        edge_ref[n] = ref[:, :WW, :]
        last_ref[n] = ref[:, count * WW :, :]


def rim_kernel(shift_ref, halo_ref, edge_ref, wq_ref, wp_ref, gain_ref, *refs):
    def spans(which, n):
        return pair_rows(halo_ref[which], edge_ref[which])

    for _ in project_windows(
        shift_ref, 0, 1, spans, wq_ref, wp_ref, gain_ref, refs[-6:-1], refs[-1]
    ):
        pass


def projected_shapes(count, c):
    return [
        jax.ShapeDtypeStruct((count, WIN, c), BF),
        jax.ShapeDtypeStruct((count, WIN, c), BF),
        jax.ShapeDtypeStruct((c, count * WIN), BF),
        jax.ShapeDtypeStruct((count, WIN, 3 * c), BF),
        jax.ShapeDtypeStruct((count, WIN, c), BF),
    ]


def before(shift, rel_index, table, gain, x, d, w_qkv, w_proj):
    c = x.shape[-1]
    count = x.shape[1] // WW
    scalar = pl.BlockSpec(memory_space=pltpu.SMEM)
    whole = pl.BlockSpec(memory_space=pltpu.VMEM)
    far = pl.BlockSpec(memory_space=pltpu.HBM)
    width = SPANS * LANES
    return pl.pallas_call(
        before_kernel,
        in_specs=[scalar, whole, whole, whole, far, far, far, far],
        out_shape=[pltpu.VMEM(o.shape, o.dtype) for o in projected_shapes(count, c)]
        + [
            pltpu.VMEM(w_qkv.shape, BF),
            pltpu.VMEM(w_proj.shape, BF),
            pltpu.VMEM((2, WH, WW, c), BF),
            pltpu.VMEM((2, WH, WW, c), BF),
            pltpu.VMEM((table.shape[1], width), BF),
            pltpu.VMEM((H, WIN, WIN), F32),
        ],
        scratch_shapes=[
            pltpu.VMEM(x.shape, BF),
            pltpu.VMEM(d.shape, BF),
            pltpu.VMEM(((count - 1) * WIN, c), BF),
            pltpu.VMEM((WIN, WIN), F32),
            pltpu.VMEM((H, width), F32),
            pltpu.SemaphoreType.DMA((4, PIECES)),
        ],
        compiler_params=FIRST_PARAMS,
        name="before",
    )(shift, rel_index, table, gain, x, d, w_qkv, w_proj)


def project_rim(shift, halo, edge, w_qkv, w_proj, gain, after, carried):
    count, _, c = carried[0].shape

    def one(array):
        return pl.BlockSpec(array.shape, lambda w: (0,) * array.ndim)

    return pl.pallas_call(
        rim_kernel,
        grid=(1,),
        in_specs=[pl.BlockSpec(memory_space=pltpu.SMEM)]
        + [one(a) for a in (halo, edge, w_qkv, w_proj, gain)]
        + [pl.BlockSpec(memory_space=pl.ANY) for _ in (after, *carried)],
        out_specs=[
            pl.BlockSpec((1, WIN, c), lambda w: (0, 0, 0)),
            pl.BlockSpec((1, WIN, c), lambda w: (0, 0, 0)),
            pl.BlockSpec((c, WIN), lambda w: (0, 0)),
            pl.BlockSpec((1, WIN, 3 * c), lambda w: (0, 0, 0)),
            pl.BlockSpec((1, WIN, c), lambda w: (0, 0, 0)),
        ],
        out_shape=projected_shapes(count, c),
        scratch_shapes=[pltpu.VMEM((WIN, c), BF)],
        input_output_aliases={7 + n: n for n in range(5)},
        compiler_params=PARAMS,
        name="project_rim",
    )(shift, halo, edge, w_qkv, w_proj, gain, after, *carried)


def own_blocks(turned):
    rows = []
    for a in range(SLAB):
        part = turned[a * HD : (a + 1) * HD]
        gap = jnp.zeros_like(part)
        rows.append(jnp.concatenate([part if b == a else gap for b in range(SLAB)], axis=1))
    return jnp.concatenate(rows, axis=0)


def own_lanes(slab):
    lane = lax.broadcasted_iota(jnp.int32, slab.shape, 1)
    return jnp.concatenate(
        [jnp.where(lane // HD == a, slab, jnp.zeros_like(slab)) for a in range(SLAB)], axis=0
    )


def attend_scores(q, k, v, dh):
    return dot(k, own_blocks(q.T)), dot(v, own_blocks(dh.T))


def attend_soft(scores, d_soft, bias_ref, sum_ref, first):
    factor = HD ** (-0.5)
    soft_all, d_all = [], []
    for a in range(SLAB):
        lanes = slice(a * WIN, (a + 1) * WIN)
        score = scores[:, lanes] * (factor * LOG2E) + bias_ref[first + a]
        raised = jnp.exp2(score - jnp.max(score, axis=0, keepdims=True))
        attention = raised * (1.0 / jnp.sum(raised, axis=0, keepdims=True))
        soft_all.append(attention.astype(BF))
        soft = d_soft[:, lanes]
        d_score = attention * (soft - jnp.sum(attention * soft, axis=0, keepdims=True))
        sum_ref[first + a] += d_score
        d_all.append(d_score.astype(BF))
    return soft_all, d_all


def attend_grads(q, k, v, dh, soft_all, d_all):
    factor = HD ** (-0.5)
    k_turned, v_turned = k.T, v.T
    att, dq = [], []
    for a in range(SLAB):
        part = slice(a * HD, (a + 1) * HD)
        att.append(dot(v_turned[part], soft_all[a]))
        dq.append(dot(k_turned[part], d_all[a]))
    att = jnp.concatenate(att, axis=0).astype(BF)
    dq = (jnp.concatenate(dq, axis=0) * factor).astype(BF).T
    dk = (dot(jnp.concatenate(d_all, axis=1), own_lanes(q)) * factor).astype(BF)
    dv = dot(jnp.concatenate(soft_all, axis=1), own_lanes(dh)).astype(BF)
    return att, dq, dk, dv


def fold_table(sum_ref, hot_ref, row_ref, heads):
    odd = odd_lanes(WH)
    for h in range(heads):
        sums = [None, None]
        for col in range(WW):
            tile = sum_ref[h, pl.ds(col, WH, stride=WW), :]
            for parity in range(2):
                kept = jnp.where(odd, tile, 0.0) if parity else jnp.where(odd, 0.0, tile)
                moved = pltpu.roll(kept, (WW - 1 - col - WW * parity) % LANES, 1)
                sums[parity] = moved if col == 0 else sums[parity] + moved
        for parity in range(2):
            row_ref[h, parity * WH : (parity + 1) * WH, :] = sums[parity]
    spans = []
    for first in range(SPANS):
        span = None
        for parity in range(2):
            row = parity + WH - 1 - first
            if 0 <= row < WH:
                part = row_ref[:, parity * WH + row, :]
                span = part if span is None else span + part
        spans.append(span)
    return joined3(dot_nt(split3(jnp.concatenate(spans, axis=1)), hot_ref[...]))


def attend_windows(windows, origin, qkv_ref, dh_ref, bias_ref, sum_ref, dp_ref, att_ref):
    c = dh_ref.shape[-1]
    slabs = c // LANES
    start, stop = windows
    together = math.gcd(stop - start, max(1, CHAINS // slabs))

    def some(n, carry):
        pieces, operands = [], []
        for m in range(together):
            for s in range(slabs):
                w = start + n * together + m
                at = s * LANES
                pieces.append((w, s))
                operands.append(
                    [qkv_ref[w, :, i * c + at : i * c + at + LANES] for i in range(3)]
                    + [dh_ref[w, :, at : at + LANES]]
                )
        scores = [attend_scores(*o) for o in operands]
        softs = [
            attend_soft(*scores[i], bias_ref, sum_ref, s * SLAB)
            for i, (_, s) in enumerate(pieces)
        ]
        for i, (w, s) in enumerate(pieces):
            att, dq, dk, dv = attend_grads(*operands[i], *softs[i])
            lanes = slice(s * LANES, (s + 1) * LANES)
            tokens = pl.ds(pl.multiple_of((w - origin) * WIN, WIN), WIN)
            att_ref[lanes, tokens] = att
            for k, part in enumerate((dq, dk, dv)):
                dp_ref[w - origin, :, k * c + s * LANES : k * c + (s + 1) * LANES] = part
        return carry

    lax.fori_loop(0, (stop - start) // together, some, 0)


def attend_first_kernel(start, qkv_ref, dh_ref, bias_ref, dp_ref, att_ref, sum_ref):
    sum_ref[...] = jnp.zeros_like(sum_ref)
    windows = (start, dh_ref.shape[0])
    attend_windows(windows, start, qkv_ref, dh_ref, bias_ref, sum_ref, dp_ref, att_ref)


def attend_first(start, qkv, dh, bias):
    count, _, c = dh.shape
    whole = pl.BlockSpec(memory_space=pltpu.VMEM)
    return pl.pallas_call(
        lambda *refs: attend_first_kernel(start, *refs),
        in_specs=[whole] * 3,
        out_shape=(
            jax.ShapeDtypeStruct((count - start, WIN, 3 * c), BF),
            jax.ShapeDtypeStruct((c, (count - start) * WIN), BF),
            jax.ShapeDtypeStruct(bias.shape, F32),
        ),
        compiler_params=PARAMS,
        name="attend_first",
    )(qkv, dh, bias)


def attend_kernel(scales, split, *refs):
    qkv_ref, dh_ref, bias_ref, hot_ref, nt_ref, d_ref, dp0_ref, att0_ref, sum0_ref = refs[:9]
    refs = refs[3:]
    dp_ref = refs[6]
    att_ref, sum_ref, row_ref = refs[-3:]
    count, _, c = dh_ref.shape
    slabs = c // LANES
    heads = slabs * SLAB
    tokens = count * WIN
    start = count - dp0_ref.shape[0]
    sum_ref[...] = sum0_ref[...]
    attend_windows((0, start), 0, qkv_ref, dh_ref, bias_ref, sum_ref, dp_ref, att_ref)
    dp_ref[start:] = dp0_ref[...]
    att_ref[:, start * WIN :] = att0_ref[...]
    grad_scale, table_scale = scales
    table = fold_table(sum_ref, hot_ref, row_ref, heads) * table_scale
    d_rows = d_ref[...].reshape(tokens, c)
    if not split:
        grad_ref, proj_ref, table_ref = refs[7:10]
        for n in range(3 * slabs):
            cols = slice(n * LANES, (n + 1) * LANES)
            part = dp_ref[:, :, cols].reshape(tokens, LANES)
            grad_ref[:, cols] = (dot(nt_ref[...], part) * grad_scale).astype(BF)
        proj_ref[...] = (dot(att_ref[...], d_rows) * grad_scale).astype(BF)
        table_ref[...] = table
        return
    kept_ref, sent_ref, table_ref, both_ref = refs[7:11]
    core = device_bits(0, 1)
    low = 2 * kept_ref.shape[0]
    top = c // (low * UNIT)
    per_top = 3 * slabs
    for n in range(0, per_top, 2):
        wide_n = min(2, per_top - n)
        part = dp_ref[:, :, n * LANES : (n + wide_n) * LANES].reshape(tokens, wide_n * LANES)
        grad = (dot(nt_ref[...], part) * grad_scale).astype(BF)
        for t in range(top):
            for b in range(low):
                row = (t * low + b) * UNIT
                for m in range(wide_n):
                    both_ref[(b % 2) ^ core, b // 2, t * per_top + n + m] = grad[
                        row : row + UNIT, m * LANES : (m + 1) * LANES
                    ]
    tiles = c // LANES
    grad = (dot(att_ref[...], d_rows) * grad_scale).astype(BF)
    for s in range(slabs):
        for b in range(low):
            row = (s * low + b) * UNIT
            for m in range(tiles):
                both_ref[(b % 2) ^ core, b // 2, top * per_top + s * tiles + m] = grad[
                    row : row + UNIT, m * LANES : (m + 1) * LANES
                ]
    table_ref[...] = jnp.zeros_like(table_ref)
    entries = table.shape[1]
    for s in range(slabs):
        for n in range(UNIT // SLAB):
            lanes = min(LANES, entries - n * LANES)
            table_ref[s, n * SLAB : (n + 1) * SLAB, :lanes] = table[
                s * SLAB : (s + 1) * SLAB, n * LANES : n * LANES + lanes
            ]
    kept_ref[...] = both_ref[0]
    units = kept_ref.shape[0] * kept_ref.shape[1]
    sent_ref[:units] = both_ref[1].reshape(units, UNIT, LANES)
    sent_ref[units:] = table_ref[...].astype(BF)


def attend(qkv, dh, bias, hot, nt, d, early, scales, n_dev, split):
    count, _, c = dh.shape
    slabs = c // LANES
    heads = slabs * SLAB
    tokens = count * WIN
    entries = hot.shape[0]
    outs = [jax.ShapeDtypeStruct((count, WIN, 3 * c), BF)]
    scratch = []
    if split:
        low = n_dev // slabs
        units = slabs * 4 * slabs
        outs += [
            jax.ShapeDtypeStruct((low // 2, units, UNIT, LANES), BF),
            jax.ShapeDtypeStruct((low // 2 * units + slabs, UNIT, LANES), BF),
            jax.ShapeDtypeStruct((slabs, UNIT, LANES), F32),
        ]
        scratch = [pltpu.VMEM((2, low // 2, units, UNIT, LANES), BF)]
    else:
        outs += [
            jax.ShapeDtypeStruct((c, 3 * c), BF),
            jax.ShapeDtypeStruct((c, c), BF),
            jax.ShapeDtypeStruct((heads, entries), F32),
        ]
    whole = pl.BlockSpec(memory_space=pltpu.VMEM)
    return pl.pallas_call(
        lambda *refs: attend_kernel(scales, split, *refs),
        in_specs=[whole] * 9,
        out_shape=outs,
        scratch_shapes=scratch
        + [
            pltpu.VMEM((c, tokens), BF),
            pltpu.VMEM((heads, WIN, WIN), F32),
            pltpu.VMEM((heads, 2 * WH, LANES), F32),
        ],
        compiler_params=PARAMS,
        name="attend",
    )(qkv, dh, bias, hot, nt, d, *early)


def input_rows(dp_ref, windows, x_ref, d_ref, w_ref, gain_ref, store):
    c = x_ref.shape[-1]
    start, stop = windows
    d_normed = None
    for n in range(3):
        part = dp_ref[start:stop, :, n * c : (n + 1) * c].reshape((stop - start) * WIN, c)
        part = dot_nt(part, w_ref[:, n * c : (n + 1) * c])
        d_normed = part if d_normed is None else d_normed + part
    for w in range(start, stop):
        grad = d_normed[(w - start) * WIN : (w - start + 1) * WIN]
        normal, inv_std = norm_stats(x_ref[w].astype(F32))
        scaled = grad * gain_ref[...]
        branch = inv_std * (
            scaled
            - jnp.mean(scaled, axis=-1, keepdims=True)
            - normal * jnp.mean(scaled * normal, axis=-1, keepdims=True)
        )
        store(w, (d_ref[w].astype(F32) + branch).astype(BF))


def input_rim_kernel(dp_ref, x_ref, d_ref, w_ref, gain_ref, out_ref):
    def store(w, value):
        out_ref[...] = value

    input_rows(dp_ref, (0, 1), x_ref, d_ref, w_ref, gain_ref, store)


def placed(select, first, second):
    c = first.shape[-1]
    pair = pair_rows(first.reshape(WH, WW, c), second.reshape(WH, WW, c))
    return dot(select, pair).astype(BF).reshape(WH, WW, c)


def input_rest_kernel(
    shift_ref, dp_ref, x_ref, d_ref, w_ref, gain_ref, rim_ref, out_ref, end_ref, row_ref
):
    count = x_ref.shape[0]
    select = shift_matrix(shift_ref[0])
    row_ref[0] = rim_ref[...]

    def store(w, value):
        row_ref[w] = value

    half = (count + 1) // 2
    for windows in ((1, half), (half, count)):
        input_rows(dp_ref, windows, x_ref, d_ref, w_ref, gain_ref, store)
        for w in range(windows[0], windows[1]):
            out_ref[:, (w - 1) * WW : w * WW, :] = placed(select, row_ref[w - 1], row_ref[w])
    end_ref[...] = row_ref[count - 1]


def place_kernel(shift_ref, end_ref, rim_ref, grid_ref, out_ref):
    out_ref[...] = placed(shift_matrix(shift_ref[0]), end_ref[...], rim_ref[...])


def input_rim(dp, x, d, w_qkv, gain):
    return pl.pallas_call(
        input_rim_kernel,
        out_shape=jax.ShapeDtypeStruct(x.shape[1:], BF),
        compiler_params=PARAMS,
        name="input_rim",
    )(dp, x, d, w_qkv, gain)


def input_rest(shift, dp, x, d, w_qkv, gain, rim):
    count, _, c = x.shape
    whole = pl.BlockSpec(memory_space=pltpu.VMEM)
    return pl.pallas_call(
        input_rest_kernel,
        in_specs=[pl.BlockSpec(memory_space=pltpu.SMEM)] + [whole] * 6,
        out_shape=(
            jax.ShapeDtypeStruct((WH, count * WW, c), BF),
            jax.ShapeDtypeStruct((WIN, c), BF),
        ),
        scratch_shapes=[pltpu.VMEM((count, WIN, c), BF)],
        compiler_params=PARAMS,
        name="input_rest",
    )(shift, dp, x, d, w_qkv, gain, rim)


def place_last(shift, end, rim, grid):
    last = grid.shape[1] // WW - 1
    c = grid.shape[2]
    one = pl.BlockSpec((WIN, c), lambda n: (0, 0))
    return pl.pallas_call(
        place_kernel,
        grid=(1,),
        in_specs=[
            pl.BlockSpec(memory_space=pltpu.SMEM),
            one,
            one,
            pl.BlockSpec(memory_space=pl.ANY),
        ],
        out_specs=pl.BlockSpec((WH, WW, c), lambda n: (0, last, 0)),
        out_shape=jax.ShapeDtypeStruct(grid.shape, BF),
        input_output_aliases={3: 0},
        compiler_params=PARAMS,
        name="place_last",
    )(shift, end, rim, grid)


def pair_sum(own, parts):
    if len(parts) == 1:
        return own + parts[0]
    return (own + parts[0]) + (parts[1] + parts[2])


def shape_of(*shape, kind=BF):
    return jax.ShapeDtypeStruct((*shape, UNIT, LANES), kind)


def stage_call(kernel, outs, *args, scratch=()):
    whole = pl.BlockSpec(memory_space=pltpu.VMEM)
    return pl.pallas_call(
        kernel,
        in_specs=[whole] * len(args),
        out_shape=outs,
        scratch_shapes=scratch,
        compiler_params=PARAMS,
    )(*args)


def core_kernel(kept_ref, got_ref, table_ref, own_a, sent_a, own_b, sent_b, out_ref):
    units = kept_ref.shape[1]
    half = units // 2
    table = table_ref[...].astype(BF).astype(F32) + got_ref[4 * units :].astype(F32)
    out_ref[...] = table
    x, y = device_bits(1, 1), device_bits(2, 1)

    def total(y, x, start):
        b = 2 * y + x
        got = got_ref[pl.ds(b * units + start, half)]
        return kept_ref[b, start : start + half].astype(F32) + got.astype(F32)

    for n in range(2):
        own_a[n] = total(n, x, 0)
        sent_a[n * half : (n + 1) * half] = total(n, 1 - x, 0).astype(BF)
        own_b[n] = total(y, n, half)
        sent_b[n * half : (n + 1) * half] = total(1 - y, n, half).astype(BF)
    sent_a[2 * half :] = table.astype(BF)


def core_stage(kept, got, table):
    half, tables = kept.shape[1] // 2, table.shape[0]
    outs = (
        shape_of(2, half, kind=F32),
        shape_of(2 * half + tables),
        shape_of(2, half, kind=F32),
        shape_of(2 * half),
        shape_of(tables, kind=F32),
    )
    return stage_call(core_kernel, outs, kept, got, table)


def pair_kernel(own_a, got_a, own_b, got_b, table_ref, keep_a, sent_a, keep_b, sent_b, out_ref):
    half = own_a.shape[1]
    table = table_ref[...].astype(BF).astype(F32) + got_a[2 * half :].astype(F32)
    out_ref[...] = table
    for own, got, keep, sent, mine in (
        (own_a, got_a, keep_a, sent_a, device_bits(2, 1)),
        (own_b, got_b, keep_b, sent_b, device_bits(1, 1)),
    ):
        keep[...] = own[mine] + got[pl.ds(mine * half, half)].astype(F32)
        other = 1 - mine
        total = own[other] + got[pl.ds(other * half, half)].astype(F32)
        sent[:half] = total.astype(BF)
    sent_a[half:] = table.astype(BF)


def pair_stage(own_a, got_a, own_b, got_b, table):
    half, tables = own_a.shape[1], table.shape[0]
    outs = (
        shape_of(half, kind=F32),
        shape_of(half + tables),
        shape_of(half, kind=F32),
        shape_of(half),
        shape_of(tables, kind=F32),
    )
    return stage_call(pair_kernel, outs, own_a, got_a, own_b, got_b, table)


def top_kernel(own_a, got_a, own_b, got_b, table_ref, kept_ref, sent1, sent2, sent3, out_ref, sum_ref):
    half = own_a.shape[0]
    sum_ref[:half] = own_a[...] + got_a[:half].astype(F32)
    sum_ref[half:] = own_b[...] + got_b[...].astype(F32)
    table = table_ref[...].astype(BF).astype(F32) + got_a[half:].astype(F32)
    out_ref[...] = table
    top = 4
    count = kept_ref.shape[0]
    tiles = count // 4
    mine = device_bits(3, 2)
    for n, target in enumerate((kept_ref, sent1, sent2, sent3)):
        t = mine ^ n
        kind = target.dtype
        target[: 3 * tiles] = sum_ref[pl.ds(t * 3 * tiles, 3 * tiles)].astype(kind)
        proj = sum_ref[pl.ds(top * 3 * tiles + t * tiles, tiles)]
        target[3 * tiles : count] = proj.astype(kind)
        if n:
            target[count:] = table.astype(BF)


def top_stage(own_a, got_a, own_b, got_b, table):
    units, tables = 2 * own_a.shape[0], table.shape[0]
    sent = shape_of(units // 4 + tables)
    outs = (shape_of(units // 4, kind=F32), sent, sent, sent, shape_of(tables, kind=F32))
    scratch = [pltpu.VMEM((units, UNIT, LANES), F32)]
    return stage_call(top_kernel, outs, own_a, got_a, own_b, got_b, table, scratch=scratch)


def finish_kernel(
    own_ref, table_ref, got1, got2, got3, w_ref, gain_ref, qkv_ref, proj_ref, g_ref, t_ref
):
    gots = (got1, got2, got3)
    units = own_ref.shape[0]
    c = proj_ref.shape[1]
    tiles = c // LANES
    entries = t_ref.shape[1]
    total = pair_sum(own_ref[...], [g[:units].astype(F32) for g in gots])
    table = pair_sum(table_ref[...].astype(BF).astype(F32), [g[units:].astype(F32) for g in gots])
    for n in range(3 * tiles):
        qkv_ref[:, n * LANES : (n + 1) * LANES] = total[n]
    for n in range(tiles):
        proj_ref[:, n * LANES : (n + 1) * LANES] = total[3 * tiles + n]
    for s in range(table.shape[0]):
        for n in range(UNIT // SLAB):
            lanes = min(LANES, entries - n * LANES)
            t_ref[s * SLAB : (s + 1) * SLAB, n * LANES : n * LANES + lanes] = table[
                s, n * SLAB : (n + 1) * SLAB, :lanes
            ]
    start = pl.multiple_of(device_index() * UNIT, UNIT)
    rows = w_ref[pl.ds(start, UNIT), :].astype(F32)
    products = jnp.sum(rows * qkv_ref[...], axis=1, keepdims=True)
    lane = lax.broadcasted_iota(jnp.int32, (UNIT, c), 1)
    row = lax.broadcasted_iota(jnp.int32, (UNIT, c), 0)
    gains = jnp.where(lane == start + row, gain_ref[...], 0.0)
    column = products / jnp.sum(gains, axis=1, keepdims=True)
    g_ref[...] = jnp.broadcast_to(column, (UNIT, LANES)).T[:1, :]


def finish(own, table, gots, w_qkv, gain, entries):
    c = w_qkv.shape[0]
    outs = (
        jax.ShapeDtypeStruct((UNIT, 3 * c), F32),
        jax.ShapeDtypeStruct((UNIT, c), F32),
        jax.ShapeDtypeStruct((1, UNIT), F32),
        jax.ShapeDtypeStruct((H, entries), F32),
    )
    return stage_call(finish_kernel, outs, own, table, *gots, w_qkv, gain)


def flat_permute(value, mask):
    total = lax.axis_size("lon") * lax.axis_size("lat")
    return lax.ppermute(value, ("lon", "lat"), [(n, n ^ mask) for n in range(total)])


def bit_groups(total):
    bits = total.bit_length() - 1
    sizes = [1]
    while sum(sizes) < bits:
        sizes.append(min(2, bits - sum(sizes)))
    return sizes


def scatter_sum(matrix):
    n_lat = lax.axis_size("lat")
    total = lax.axis_size("lon") * n_lat
    me = lax.axis_index("lon") * n_lat + lax.axis_index("lat")
    rows, cols = matrix.shape
    blocks = matrix.reshape(total, rows // total, cols)
    low = 0
    sizes = bit_groups(total)
    for size in sizes:
        ways = 1 << size
        mine = (me >> low) & (ways - 1)
        view = blocks.reshape(blocks.shape[0] // ways, ways, rows // total, cols)
        kept = lax.dynamic_index_in_dim(view, mine, 1, keepdims=False).astype(F32)
        for n in range(1, ways):
            sent = lax.dynamic_index_in_dim(view, mine ^ n, 1, keepdims=False)
            kept = kept + flat_permute(sent, n << low).astype(F32)
        low += size
        blocks = kept if low == sum(sizes) else kept.astype(BF)
    return blocks.reshape(rows // total, cols)


def full_sum(value):
    total = lax.axis_size("lon") * lax.axis_size("lat")
    low = 0
    for size in bit_groups(total):
        value = pair_sum(value, [flat_permute(value, n << low) for n in range(1, 1 << size)])
        low += size
    return value


def ring_shift(value, steps):
    count = lax.axis_size("lon")
    return lax.ppermute(value, "lon", [(n, (n + steps) % count) for n in range(count)])


def step(inputs, d_out, w_qkv, w_proj, gain, bias_table, rel_index, shifts):
    n_lon = lax.axis_size("lon")
    n_lat = lax.axis_size("lat")
    n_dev = n_lon * n_lat
    _, columns, c = inputs.shape
    tokens = inputs.shape[0] * columns * n_dev
    scales = (tokens ** (-0.5), (tokens // WIN) ** (-0.5))
    entries = bias_table.shape[0]
    gain_row = gain.reshape(1, c)
    split = c // n_dev == UNIT and n_lat == 4

    *carried, w_qkv, w_proj, edge, last, hot, bias = before(
        shifts, rel_index, bias_table.T, gain_row, inputs, d_out, w_qkv, w_proj
    )
    halo = ring_shift(last, 1)
    early = attend_first(EARLY, carried[3], carried[4], bias)
    x, d, nt, qkv, dh = project_rim(shifts, halo, edge, w_qkv, w_proj, gain_row, early[2], carried)
    dp, *out = attend(qkv, dh, bias, hot, nt, d, early, scales, n_dev, split)
    if split:
        kept, sent, table = out
        got = flat_permute(sent, 1)
    first = input_rim(dp, x, d, w_qkv, gain_row)
    returned = ring_shift(first, -1)
    if split:
        own_a, sent_a, own_b, sent_b, table = core_stage(kept, got, table)
        got_a, got_b = flat_permute(sent_a, 2), flat_permute(sent_b, 4)
    grid, end = input_rest(shifts, dp, x, d, w_qkv, gain_row, first)
    if split:
        own_a, sent_a, own_b, sent_b, table = pair_stage(own_a, got_a, own_b, got_b, table)
        got_a, got_b = flat_permute(sent_a, 4), flat_permute(sent_b, 2)
    d_inputs = place_last(shifts, end, returned, grid)
    if split:
        own, *sent, table = top_stage(own_a, got_a, own_b, got_b, table)
        gots = [flat_permute(value, n << 3) for n, value in enumerate(sent, 1)]
        g_qkv, g_proj, g_gain, g_table = finish(own, table, gots, w_qkv, gain_row, entries)
        return (d_inputs, g_qkv, g_proj, g_gain.reshape(UNIT), g_table.T)

    own = scatter_sum(jnp.concatenate(out[:2], axis=1))
    g_qkv, g_proj = own[:, : 3 * c], own[:, 3 * c :]
    g_table = full_sum(out[2]).T
    rows = c // n_dev
    me = device_index()
    w_rows = lax.dynamic_slice_in_dim(w_qkv, me * rows, rows, 0).astype(F32)
    gain_rows = lax.dynamic_slice_in_dim(gain, me * rows, rows, 0)
    g_gain = jnp.sum(w_rows * g_qkv, axis=1) / gain_rows
    return (d_inputs, g_qkv, g_proj, g_gain, g_table)


def solution(mesh):
    return jax.shard_map(
        step,
        mesh=mesh,
        in_specs=(P("lat", "lon", None), P("lat", "lon", None), P(), P(), P(), P(), P(), P("lat")),
        out_specs=(
            P("lat", "lon", None),
            P(("lon", "lat"), None),
            P(("lon", "lat"), None),
            P(("lon", "lat")),
            P(),
        ),
        check_vma=False,
    )
```

```python
import math

import jax
import jax.numpy as jnp
from jax import lax
from jax.experimental import pallas as pl
from jax.experimental.pallas import tpu as pltpu
from jax.sharding import PartitionSpec as P


H = 16
HD = 32
WH = 8
WW = 16
WIN = WH * WW
LANES = 128
SLAB = LANES // HD
SPANS = WH + 1
UNIT = 16
PIECES = 1
EARLY = 2
SHARE = 5
CHAINS = 16
EPSILON = 1e-05
LOG2E = math.log2(math.e)
BF = jnp.bfloat16
F32 = jnp.float32
PARAMS = pltpu.CompilerParams(vmem_limit_bytes=24 * 2**20)
FIRST_PARAMS = pltpu.CompilerParams(vmem_limit_bytes=49 * 2**20)


def dot(left, right):
    return lax.dot_general(left, right, (((1,), (0,)), ((), ())), preferred_element_type=F32)


def dot_nt(left, right):
    return lax.dot_general(left, right, (((1,), (1,)), ((), ())), preferred_element_type=F32)


def split3(value):
    high = value.astype(BF)
    rest = value - high.astype(F32)
    middle = rest.astype(BF)
    low = (rest - middle.astype(F32)).astype(BF)
    return jnp.concatenate([high, middle, low], axis=0)


def joined3(value):
    rows = value.shape[0] // 3
    return (value[:rows] + value[rows : 2 * rows]) + value[2 * rows :]


def device_index():
    return lax.axis_index("lon") * lax.axis_size("lat") + lax.axis_index("lat")


def device_bits(low, size):
    return lax.shift_right_logical(device_index(), low) & ((1 << size) - 1)


def odd_lanes(rows):
    lane = lax.broadcasted_iota(jnp.int32, (rows, LANES), 1)
    return (lane // WW) % 2 == 1


def fill_bias(rel_ref, table_ref, hot_ref, bias_ref, line_ref, span_ref):
    line_ref[...] = rel_ref[...].astype(F32).T
    slot = lax.broadcasted_iota(jnp.int32, (1, LANES), 1) % (2 * WW)
    codes = []
    for first in range(SPANS):
        row = max(WH - 1 - first, 0)
        parity = first + row - (WH - 1)
        near = line_ref[row * WW + WW - 1 : row * WW + WW, :]
        far = line_ref[row * WW : row * WW + 1, :]
        if parity:
            near = pltpu.roll(near, LANES - WW, 1)
        far = pltpu.roll(far, (WW - 1 - WW * parity) % LANES, 1)
        code = jnp.where(slot < WW, near, far)
        codes.append(jnp.where(slot == 2 * WW - 1, -1.0, code))
    code = jnp.concatenate(codes, axis=1).astype(jnp.int32)
    entry = lax.broadcasted_iota(jnp.int32, hot_ref.shape, 0)
    hot = jnp.where(entry == code, 1.0, 0.0).astype(BF)
    hot_ref[...] = hot
    span_ref[...] = joined3(dot(split3(table_ref[...]), hot)) * LOG2E
    odd = odd_lanes(WW)
    for h in range(H):
        for row in range(WH):
            halves = []
            for parity in range(2):
                first = parity - row + WH - 1
                line = span_ref[h : h + 1, first * LANES : (first + 1) * LANES]
                line = jnp.broadcast_to(line, (WW, LANES))
                turn = (LANES - (WW - 1) + WW * parity) % LANES
                halves.append(pltpu.roll(line, turn, 1, stride=1, stride_axis=0))
            bias_ref[h, row * WW : (row + 1) * WW, :] = jnp.where(odd, halves[1], halves[0])


def norm_stats(rows):
    centred = rows - jnp.mean(rows, axis=-1, keepdims=True)
    inv_std = lax.rsqrt(jnp.mean(centred * centred, axis=-1, keepdims=True) + EPSILON)
    return centred * inv_std, inv_std


def pair_rows(first, second):
    both = jnp.concatenate([first, second], axis=1)
    return both.reshape(both.shape[0] * both.shape[1], both.shape[2])


def shift_matrix(offset):
    row = lax.broadcasted_iota(jnp.int32, (WIN, 2 * WIN), 0)
    col = lax.broadcasted_iota(jnp.int32, (WIN, 2 * WIN), 1)
    same = (row // WW) == (col // (2 * WW))
    hit = same & ((col % (2 * WW)) == (row % WW) + offset)
    return jnp.where(hit, 1.0, 0.0).astype(BF)


def project_windows(shift_ref, first, count, spans, wq_ref, wp_ref, gain_ref, outs, norm_ref):
    xw_ref, dw_ref, nt_ref, qkv_ref, dh_ref = outs
    c = wq_ref.shape[0]
    tokens = count * WIN
    select = shift_matrix(WW - shift_ref[0])
    for n in range(count):
        rows = slice(n * WIN, (n + 1) * WIN)
        values = dot(select, spans(0, n))
        xw_ref[first + n] = values.astype(BF)
        normal, _ = norm_stats(values)
        normed = (normal * gain_ref[...]).astype(BF)
        norm_ref[rows, :] = normed
        nt_ref[:, (first + n) * WIN : (first + n + 1) * WIN] = normed.T
    yield
    for n in range(count):
        dw_ref[first + n] = dot(select, spans(1, n)).astype(BF)
    yield
    step = 2 * LANES
    for n in range(3 * c // step):
        cols = slice(n * step, (n + 1) * step)
        part = dot(norm_ref[...], wq_ref[:, cols]).astype(BF)
        qkv_ref[first:, :, cols] = part.reshape(count, WIN, step)
    yield
    grads = dw_ref[first:].reshape(tokens, c)
    for n in range(c // step):
        cols = slice(n * step, (n + 1) * step)
        part = dot_nt(grads, wp_ref[cols, :]).astype(BF)
        dh_ref[first:, :, cols] = part.reshape(count, WIN, step)
    yield


def before_kernel(shift_ref, rel_ref, table_ref, gain_ref, x_hbm, d_hbm, wq_hbm, wp_hbm, *refs):
    outs, (wq_ref, wp_ref, edge_ref, last_ref, hot_ref, bias_ref) = refs[:5], refs[5:11]
    x_ref, d_ref, norm_ref, line_ref, span_ref, sems = refs[11:]
    pairs = ((x_hbm, x_ref), (d_hbm, d_ref), (wq_hbm, wq_ref), (wp_hbm, wp_ref))
    copies = []
    for n, (source, target) in enumerate(pairs):
        rows = source.shape[0] // PIECES
        parts = [pl.ds(m * rows, rows) for m in range(PIECES)]
        copies.append(
            [
                pltpu.make_async_copy(source.at[part], target.at[part], sems.at[n, m])
                for m, part in enumerate(parts)
            ]
        )
    for group in copies:
        for copy in group:
            copy.start()
    fill_bias(rel_ref, table_ref, hot_ref, bias_ref, line_ref, span_ref)
    count = x_ref.shape[1] // WW - 1

    def spans(which, n):
        ref = (x_ref, d_ref)[which]
        return pair_rows(ref[:, n * WW : (n + 1) * WW, :], ref[:, (n + 1) * WW : (n + 2) * WW, :])

    stages = project_windows(shift_ref, 1, count, spans, wq_ref, wp_ref, gain_ref, outs, norm_ref)
    for group in copies:
        for copy in group:
            copy.wait()
        next(stages)
    for n, ref in enumerate((x_ref, d_ref)):
        edge_ref[n] = ref[:, :WW, :]
        last_ref[n] = ref[:, count * WW :, :]


def rim_kernel(shift_ref, halo_ref, edge_ref, wq_ref, wp_ref, gain_ref, *refs):
    def spans(which, n):
        return pair_rows(halo_ref[which], edge_ref[which])

    for _ in project_windows(
        shift_ref, 0, 1, spans, wq_ref, wp_ref, gain_ref, refs[-6:-1], refs[-1]
    ):
        pass


def projected_shapes(count, c):
    return [
        jax.ShapeDtypeStruct((count, WIN, c), BF),
        jax.ShapeDtypeStruct((count, WIN, c), BF),
        jax.ShapeDtypeStruct((c, count * WIN), BF),
        jax.ShapeDtypeStruct((count, WIN, 3 * c), BF),
        jax.ShapeDtypeStruct((count, WIN, c), BF),
    ]


def before(shift, rel_index, table, gain, x, d, w_qkv, w_proj):
    c = x.shape[-1]
    count = x.shape[1] // WW
    scalar = pl.BlockSpec(memory_space=pltpu.SMEM)
    whole = pl.BlockSpec(memory_space=pltpu.VMEM)
    far = pl.BlockSpec(memory_space=pltpu.HBM)
    width = SPANS * LANES
    return pl.pallas_call(
        before_kernel,
        in_specs=[scalar, whole, whole, whole, far, far, far, far],
        out_shape=[pltpu.VMEM(o.shape, o.dtype) for o in projected_shapes(count, c)]
        + [
            pltpu.VMEM(w_qkv.shape, BF),
            pltpu.VMEM(w_proj.shape, BF),
            pltpu.VMEM((2, WH, WW, c), BF),
            pltpu.VMEM((2, WH, WW, c), BF),
            pltpu.VMEM((table.shape[1], width), BF),
            pltpu.VMEM((H, WIN, WIN), F32),
        ],
        scratch_shapes=[
            pltpu.VMEM(x.shape, BF),
            pltpu.VMEM(d.shape, BF),
            pltpu.VMEM(((count - 1) * WIN, c), BF),
            pltpu.VMEM((WIN, WIN), F32),
            pltpu.VMEM((H, width), F32),
            pltpu.SemaphoreType.DMA((4, PIECES)),
        ],
        compiler_params=FIRST_PARAMS,
        name="before",
    )(shift, rel_index, table, gain, x, d, w_qkv, w_proj)


def project_rim(shift, halo, edge, w_qkv, w_proj, gain, after, carried):
    count, _, c = carried[0].shape

    def one(array):
        return pl.BlockSpec(array.shape, lambda w: (0,) * array.ndim)

    return pl.pallas_call(
        rim_kernel,
        grid=(1,),
        in_specs=[pl.BlockSpec(memory_space=pltpu.SMEM)]
        + [one(a) for a in (halo, edge, w_qkv, w_proj, gain)]
        + [pl.BlockSpec(memory_space=pl.ANY) for _ in (after, *carried)],
        out_specs=[
            pl.BlockSpec((1, WIN, c), lambda w: (0, 0, 0)),
            pl.BlockSpec((1, WIN, c), lambda w: (0, 0, 0)),
            pl.BlockSpec((c, WIN), lambda w: (0, 0)),
            pl.BlockSpec((1, WIN, 3 * c), lambda w: (0, 0, 0)),
            pl.BlockSpec((1, WIN, c), lambda w: (0, 0, 0)),
        ],
        out_shape=projected_shapes(count, c),
        scratch_shapes=[pltpu.VMEM((WIN, c), BF)],
        input_output_aliases={7 + n: n for n in range(5)},
        compiler_params=PARAMS,
        name="project_rim",
    )(shift, halo, edge, w_qkv, w_proj, gain, after, *carried)


def own_blocks(turned):
    rows = []
    for a in range(SLAB):
        part = turned[a * HD : (a + 1) * HD]
        gap = jnp.zeros_like(part)
        rows.append(jnp.concatenate([part if b == a else gap for b in range(SLAB)], axis=1))
    return jnp.concatenate(rows, axis=0)


def own_lanes(slab):
    lane = lax.broadcasted_iota(jnp.int32, slab.shape, 1)
    return jnp.concatenate(
        [jnp.where(lane // HD == a, slab, jnp.zeros_like(slab)) for a in range(SLAB)], axis=0
    )


def attend_scores(q, k, v, dh):
    return dot(k, own_blocks(q.T)), dot(v, own_blocks(dh.T))


def attend_soft(scores, d_soft, bias_ref, sum_ref, first):
    factor = HD ** (-0.5)
    soft_all, d_all = [], []
    for a in range(SLAB):
        lanes = slice(a * WIN, (a + 1) * WIN)
        score = scores[:, lanes] * (factor * LOG2E) + bias_ref[first + a]
        raised = jnp.exp2(score - jnp.max(score, axis=0, keepdims=True))
        attention = raised * (1.0 / jnp.sum(raised, axis=0, keepdims=True))
        soft_all.append(attention.astype(BF))
        soft = d_soft[:, lanes]
        d_score = attention * (soft - jnp.sum(attention * soft, axis=0, keepdims=True))
        sum_ref[first + a] += d_score
        d_all.append(d_score.astype(BF))
    return soft_all, d_all


def attend_grads(q, k, v, dh, soft_all, d_all):
    factor = HD ** (-0.5)
    k_turned, v_turned = k.T, v.T
    att, dq = [], []
    for a in range(SLAB):
        part = slice(a * HD, (a + 1) * HD)
        att.append(dot(v_turned[part], soft_all[a]))
        dq.append(dot(k_turned[part], d_all[a]))
    att = jnp.concatenate(att, axis=0).astype(BF)
    dq = (jnp.concatenate(dq, axis=0) * factor).astype(BF).T
    dk = (dot(jnp.concatenate(d_all, axis=1), own_lanes(q)) * factor).astype(BF)
    dv = dot(jnp.concatenate(soft_all, axis=1), own_lanes(dh)).astype(BF)
    return att, dq, dk, dv


def fold_table(sum_ref, hot_ref, row_ref, heads):
    odd = odd_lanes(WH)
    for h in range(heads):
        sums = [None, None]
        for col in range(WW):
            tile = sum_ref[h, pl.ds(col, WH, stride=WW), :]
            for parity in range(2):
                kept = jnp.where(odd, tile, 0.0) if parity else jnp.where(odd, 0.0, tile)
                moved = pltpu.roll(kept, (WW - 1 - col - WW * parity) % LANES, 1)
                sums[parity] = moved if col == 0 else sums[parity] + moved
        for parity in range(2):
            row_ref[h, parity * WH : (parity + 1) * WH, :] = sums[parity]
    spans = []
    for first in range(SPANS):
        span = None
        for parity in range(2):
            row = parity + WH - 1 - first
            if 0 <= row < WH:
                part = row_ref[:, parity * WH + row, :]
                span = part if span is None else span + part
        spans.append(span)
    return joined3(dot_nt(split3(jnp.concatenate(spans, axis=1)), hot_ref[...]))


def attend_windows(windows, origin, qkv_ref, dh_ref, bias_ref, sum_ref, dp_ref, att_ref):
    c = dh_ref.shape[-1]
    slabs = c // LANES
    start, stop = windows
    together = math.gcd(stop - start, max(1, CHAINS // slabs))

    def some(n, carry):
        pieces, operands = [], []
        for m in range(together):
            for s in range(slabs):
                w = start + n * together + m
                at = s * LANES
                pieces.append((w, s))
                operands.append(
                    [qkv_ref[w, :, i * c + at : i * c + at + LANES] for i in range(3)]
                    + [dh_ref[w, :, at : at + LANES]]
                )
        scores = [attend_scores(*o) for o in operands]
        softs = [
            attend_soft(*scores[i], bias_ref, sum_ref, s * SLAB)
            for i, (_, s) in enumerate(pieces)
        ]
        for i, (w, s) in enumerate(pieces):
            att, dq, dk, dv = attend_grads(*operands[i], *softs[i])
            lanes = slice(s * LANES, (s + 1) * LANES)
            tokens = pl.ds(pl.multiple_of((w - origin) * WIN, WIN), WIN)
            att_ref[lanes, tokens] = att
            for k, part in enumerate((dq, dk, dv)):
                dp_ref[w - origin, :, k * c + s * LANES : k * c + (s + 1) * LANES] = part
        return carry

    lax.fori_loop(0, (stop - start) // together, some, 0)


def attend_first_kernel(start, qkv_ref, dh_ref, bias_ref, dp_ref, att_ref, sum_ref):
    sum_ref[...] = jnp.zeros_like(sum_ref)
    windows = (start, dh_ref.shape[0])
    attend_windows(windows, start, qkv_ref, dh_ref, bias_ref, sum_ref, dp_ref, att_ref)


def attend_first(start, qkv, dh, bias):
    count, _, c = dh.shape
    whole = pl.BlockSpec(memory_space=pltpu.VMEM)
    return pl.pallas_call(
        lambda *refs: attend_first_kernel(start, *refs),
        in_specs=[whole] * 3,
        out_shape=(
            jax.ShapeDtypeStruct((count - start, WIN, 3 * c), BF),
            jax.ShapeDtypeStruct((c, (count - start) * WIN), BF),
            jax.ShapeDtypeStruct(bias.shape, F32),
        ),
        compiler_params=PARAMS,
        name="attend_first",
    )(qkv, dh, bias)


def attend_kernel(scales, split, *refs):
    qkv_ref, dh_ref, bias_ref, hot_ref, nt_ref, d_ref, dp0_ref, att0_ref, sum0_ref = refs[:9]
    refs = refs[3:]
    dp_ref = refs[6]
    att_ref, sum_ref, row_ref = refs[-3:]
    count, _, c = dh_ref.shape
    slabs = c // LANES
    heads = slabs * SLAB
    tokens = count * WIN
    start = count - dp0_ref.shape[0]
    sum_ref[...] = sum0_ref[...]
    attend_windows((0, start), 0, qkv_ref, dh_ref, bias_ref, sum_ref, dp_ref, att_ref)
    dp_ref[start:] = dp0_ref[...]
    att_ref[:, start * WIN :] = att0_ref[...]
    grad_scale, table_scale = scales
    table = fold_table(sum_ref, hot_ref, row_ref, heads) * table_scale
    d_rows = d_ref[...].reshape(tokens, c)
    if not split:
        grad_ref, proj_ref, table_ref = refs[7:10]
        for n in range(3 * slabs):
            cols = slice(n * LANES, (n + 1) * LANES)
            part = dp_ref[:, :, cols].reshape(tokens, LANES)
            grad_ref[:, cols] = (dot(nt_ref[...], part) * grad_scale).astype(BF)
        proj_ref[...] = (dot(att_ref[...], d_rows) * grad_scale).astype(BF)
        table_ref[...] = table
        return
    kept_ref, sent_ref, table_ref, both_ref = refs[7:11]
    core = device_bits(0, 1)
    low = 2 * kept_ref.shape[0]
    top = c // (low * UNIT)
    per_top = 3 * slabs
    for n in range(0, per_top, 2):
        wide_n = min(2, per_top - n)
        part = dp_ref[:, :, n * LANES : (n + wide_n) * LANES].reshape(tokens, wide_n * LANES)
        grad = (dot(nt_ref[...], part) * grad_scale).astype(BF)
        for t in range(top):
            for b in range(low):
                row = (t * low + b) * UNIT
                for m in range(wide_n):
                    both_ref[(b % 2) ^ core, b // 2, t * per_top + n + m] = grad[
                        row : row + UNIT, m * LANES : (m + 1) * LANES
                    ]
    tiles = c // LANES
    grad = (dot(att_ref[...], d_rows) * grad_scale).astype(BF)
    for s in range(slabs):
        for b in range(low):
            row = (s * low + b) * UNIT
            for m in range(tiles):
                both_ref[(b % 2) ^ core, b // 2, top * per_top + s * tiles + m] = grad[
                    row : row + UNIT, m * LANES : (m + 1) * LANES
                ]
    table_ref[...] = jnp.zeros_like(table_ref)
    entries = table.shape[1]
    for s in range(slabs):
        for n in range(UNIT // SLAB):
            lanes = min(LANES, entries - n * LANES)
            table_ref[s, n * SLAB : (n + 1) * SLAB, :lanes] = table[
                s * SLAB : (s + 1) * SLAB, n * LANES : n * LANES + lanes
            ]
    kept_ref[...] = both_ref[0]
    units = kept_ref.shape[0] * kept_ref.shape[1]
    sent_ref[:units] = both_ref[1].reshape(units, UNIT, LANES)
    sent_ref[units:] = table_ref[...].astype(BF)


def attend(qkv, dh, bias, hot, nt, d, early, scales, n_dev, split):
    count, _, c = dh.shape
    slabs = c // LANES
    heads = slabs * SLAB
    tokens = count * WIN
    entries = hot.shape[0]
    outs = [jax.ShapeDtypeStruct((count, WIN, 3 * c), BF)]
    scratch = []
    if split:
        low = n_dev // slabs
        units = slabs * 4 * slabs
        outs += [
            jax.ShapeDtypeStruct((low // 2, units, UNIT, LANES), BF),
            jax.ShapeDtypeStruct((low // 2 * units + slabs, UNIT, LANES), BF),
            jax.ShapeDtypeStruct((slabs, UNIT, LANES), F32),
        ]
        scratch = [pltpu.VMEM((2, low // 2, units, UNIT, LANES), BF)]
    else:
        outs += [
            jax.ShapeDtypeStruct((c, 3 * c), BF),
            jax.ShapeDtypeStruct((c, c), BF),
            jax.ShapeDtypeStruct((heads, entries), F32),
        ]
    whole = pl.BlockSpec(memory_space=pltpu.VMEM)
    return pl.pallas_call(
        lambda *refs: attend_kernel(scales, split, *refs),
        in_specs=[whole] * 9,
        out_shape=outs,
        scratch_shapes=scratch
        + [
            pltpu.VMEM((c, tokens), BF),
            pltpu.VMEM((heads, WIN, WIN), F32),
            pltpu.VMEM((heads, 2 * WH, LANES), F32),
        ],
        compiler_params=PARAMS,
        name="attend",
    )(qkv, dh, bias, hot, nt, d, *early)


def input_rows(dp_ref, windows, x_ref, d_ref, w_ref, gain_ref, store):
    c = x_ref.shape[-1]
    start, stop = windows
    d_normed = None
    for n in range(3):
        part = dp_ref[start:stop, :, n * c : (n + 1) * c].reshape((stop - start) * WIN, c)
        part = dot_nt(part, w_ref[:, n * c : (n + 1) * c])
        d_normed = part if d_normed is None else d_normed + part
    for w in range(start, stop):
        grad = d_normed[(w - start) * WIN : (w - start + 1) * WIN]
        normal, inv_std = norm_stats(x_ref[w].astype(F32))
        scaled = grad * gain_ref[...]
        branch = inv_std * (
            scaled
            - jnp.mean(scaled, axis=-1, keepdims=True)
            - normal * jnp.mean(scaled * normal, axis=-1, keepdims=True)
        )
        store(w, (d_ref[w].astype(F32) + branch).astype(BF))


def input_rim_kernel(dp_ref, x_ref, d_ref, w_ref, gain_ref, out_ref):
    def store(w, value):
        out_ref[...] = value

    input_rows(dp_ref, (0, 1), x_ref, d_ref, w_ref, gain_ref, store)


def placed(select, first, second):
    c = first.shape[-1]
    pair = pair_rows(first.reshape(WH, WW, c), second.reshape(WH, WW, c))
    return dot(select, pair).astype(BF).reshape(WH, WW, c)


def input_rest_kernel(
    shift_ref, dp_ref, x_ref, d_ref, w_ref, gain_ref, rim_ref, out_ref, end_ref, row_ref
):
    count = x_ref.shape[0]
    select = shift_matrix(shift_ref[0])
    row_ref[0] = rim_ref[...]

    def store(w, value):
        row_ref[w] = value

    half = (count + 1) // 2
    for windows in ((1, half), (half, count)):
        input_rows(dp_ref, windows, x_ref, d_ref, w_ref, gain_ref, store)
        for w in range(windows[0], windows[1]):
            out_ref[:, (w - 1) * WW : w * WW, :] = placed(select, row_ref[w - 1], row_ref[w])
    end_ref[...] = row_ref[count - 1]


def place_kernel(shift_ref, end_ref, rim_ref, grid_ref, out_ref):
    out_ref[...] = placed(shift_matrix(shift_ref[0]), end_ref[...], rim_ref[...])


def input_rim(dp, x, d, w_qkv, gain):
    return pl.pallas_call(
        input_rim_kernel,
        out_shape=jax.ShapeDtypeStruct(x.shape[1:], BF),
        compiler_params=PARAMS,
        name="input_rim",
    )(dp, x, d, w_qkv, gain)


def input_rest(shift, dp, x, d, w_qkv, gain, rim):
    count, _, c = x.shape
    whole = pl.BlockSpec(memory_space=pltpu.VMEM)
    return pl.pallas_call(
        input_rest_kernel,
        in_specs=[pl.BlockSpec(memory_space=pltpu.SMEM)] + [whole] * 6,
        out_shape=(
            jax.ShapeDtypeStruct((WH, count * WW, c), BF),
            jax.ShapeDtypeStruct((WIN, c), BF),
        ),
        scratch_shapes=[pltpu.VMEM((count, WIN, c), BF)],
        compiler_params=PARAMS,
        name="input_rest",
    )(shift, dp, x, d, w_qkv, gain, rim)


def place_last(shift, end, rim, grid):
    last = grid.shape[1] // WW - 1
    c = grid.shape[2]
    one = pl.BlockSpec((WIN, c), lambda n: (0, 0))
    return pl.pallas_call(
        place_kernel,
        grid=(1,),
        in_specs=[
            pl.BlockSpec(memory_space=pltpu.SMEM),
            one,
            one,
            pl.BlockSpec(memory_space=pl.ANY),
        ],
        out_specs=pl.BlockSpec((WH, WW, c), lambda n: (0, last, 0)),
        out_shape=jax.ShapeDtypeStruct(grid.shape, BF),
        input_output_aliases={3: 0},
        compiler_params=PARAMS,
        name="place_last",
    )(shift, end, rim, grid)


def pair_sum(own, parts):
    if len(parts) == 1:
        return own + parts[0]
    return (own + parts[0]) + (parts[1] + parts[2])


def shape_of(*shape, kind=BF):
    return jax.ShapeDtypeStruct((*shape, UNIT, LANES), kind)


def stage_call(kernel, outs, *args, scratch=()):
    whole = pl.BlockSpec(memory_space=pltpu.VMEM)
    return pl.pallas_call(
        kernel,
        in_specs=[whole] * len(args),
        out_shape=outs,
        scratch_shapes=scratch,
        compiler_params=PARAMS,
    )(*args)


def core_kernel(kept_ref, got_ref, table_ref, own_a, sent_a, own_b, sent_b, out_ref):
    units = kept_ref.shape[1]
    half = own_a.shape[1]
    table = table_ref[...].astype(BF).astype(F32) + got_ref[4 * units :].astype(F32)
    out_ref[...] = table
    x, y = device_bits(1, 1), device_bits(2, 1)

    rest = units - half

    def total(y, x, start, size):
        b = 2 * y + x
        got = got_ref[pl.ds(b * units + start, size)]
        return kept_ref[b, start : start + size].astype(F32) + got.astype(F32)

    for n in range(2):
        own_a[n] = total(n, x, 0, half)
        sent_a[n * half : (n + 1) * half] = total(n, 1 - x, 0, half).astype(BF)
        own_b[n] = total(y, n, half, rest)
        sent_b[n * rest : (n + 1) * rest] = total(1 - y, n, half, rest).astype(BF)
    sent_a[2 * half :] = table.astype(BF)


def core_stage(kept, got, table):
    units, tables = kept.shape[1], table.shape[0]
    half = units * SHARE // 8
    outs = (
        shape_of(2, half, kind=F32),
        shape_of(2 * half + tables),
        shape_of(2, units - half, kind=F32),
        shape_of(2 * (units - half)),
        shape_of(tables, kind=F32),
    )
    return stage_call(core_kernel, outs, kept, got, table)


def pair_kernel(own_a, got_a, own_b, got_b, table_ref, keep_a, sent_a, keep_b, sent_b, out_ref):
    half = own_a.shape[1]
    table = table_ref[...].astype(BF).astype(F32) + got_a[2 * half :].astype(F32)
    out_ref[...] = table
    for own, got, keep, sent, mine in (
        (own_a, got_a, keep_a, sent_a, device_bits(2, 1)),
        (own_b, got_b, keep_b, sent_b, device_bits(1, 1)),
    ):
        size = own.shape[1]
        keep[...] = own[mine] + got[pl.ds(mine * size, size)].astype(F32)
        other = 1 - mine
        total = own[other] + got[pl.ds(other * size, size)].astype(F32)
        sent[:size] = total.astype(BF)
    sent_a[half:] = table.astype(BF)


def pair_stage(own_a, got_a, own_b, got_b, table):
    half, rest, tables = own_a.shape[1], own_b.shape[1], table.shape[0]
    outs = (
        shape_of(half, kind=F32),
        shape_of(half + tables),
        shape_of(rest, kind=F32),
        shape_of(rest),
        shape_of(tables, kind=F32),
    )
    return stage_call(pair_kernel, outs, own_a, got_a, own_b, got_b, table)


def top_kernel(own_a, got_a, own_b, got_b, table_ref, kept_ref, sent1, sent2, sent3, out_ref, sum_ref):
    half = own_a.shape[0]
    sum_ref[:half] = own_a[...] + got_a[:half].astype(F32)
    sum_ref[half:] = own_b[...] + got_b[...].astype(F32)
    table = table_ref[...].astype(BF).astype(F32) + got_a[half:].astype(F32)
    out_ref[...] = table
    top = 4
    count = kept_ref.shape[0]
    tiles = count // 4
    mine = device_bits(3, 2)
    for n, target in enumerate((kept_ref, sent1, sent2, sent3)):
        t = mine ^ n
        kind = target.dtype
        target[: 3 * tiles] = sum_ref[pl.ds(t * 3 * tiles, 3 * tiles)].astype(kind)
        proj = sum_ref[pl.ds(top * 3 * tiles + t * tiles, tiles)]
        target[3 * tiles : count] = proj.astype(kind)
        if n:
            target[count:] = table.astype(BF)


def top_stage(own_a, got_a, own_b, got_b, table):
    units, tables = own_a.shape[0] + own_b.shape[0], table.shape[0]
    sent = shape_of(units // 4 + tables)
    outs = (shape_of(units // 4, kind=F32), sent, sent, sent, shape_of(tables, kind=F32))
    scratch = [pltpu.VMEM((units, UNIT, LANES), F32)]
    return stage_call(top_kernel, outs, own_a, got_a, own_b, got_b, table, scratch=scratch)


def finish_kernel(
    own_ref, table_ref, got1, got2, got3, w_ref, gain_ref, qkv_ref, proj_ref, g_ref, t_ref
):
    gots = (got1, got2, got3)
    units = own_ref.shape[0]
    c = proj_ref.shape[1]
    tiles = c // LANES
    entries = t_ref.shape[1]
    total = pair_sum(own_ref[...], [g[:units].astype(F32) for g in gots])
    table = pair_sum(table_ref[...].astype(BF).astype(F32), [g[units:].astype(F32) for g in gots])
    for n in range(3 * tiles):
        qkv_ref[:, n * LANES : (n + 1) * LANES] = total[n]
    for n in range(tiles):
        proj_ref[:, n * LANES : (n + 1) * LANES] = total[3 * tiles + n]
    for s in range(table.shape[0]):
        for n in range(UNIT // SLAB):
            lanes = min(LANES, entries - n * LANES)
            t_ref[s * SLAB : (s + 1) * SLAB, n * LANES : n * LANES + lanes] = table[
                s, n * SLAB : (n + 1) * SLAB, :lanes
            ]
    start = pl.multiple_of(device_index() * UNIT, UNIT)
    rows = w_ref[pl.ds(start, UNIT), :].astype(F32)
    products = jnp.sum(rows * qkv_ref[...], axis=1, keepdims=True)
    lane = lax.broadcasted_iota(jnp.int32, (UNIT, c), 1)
    row = lax.broadcasted_iota(jnp.int32, (UNIT, c), 0)
    gains = jnp.where(lane == start + row, gain_ref[...], 0.0)
    column = products / jnp.sum(gains, axis=1, keepdims=True)
    g_ref[...] = jnp.broadcast_to(column, (UNIT, LANES)).T[:1, :]


def finish(own, table, gots, w_qkv, gain, entries):
    c = w_qkv.shape[0]
    outs = (
        jax.ShapeDtypeStruct((UNIT, 3 * c), F32),
        jax.ShapeDtypeStruct((UNIT, c), F32),
        jax.ShapeDtypeStruct((1, UNIT), F32),
        jax.ShapeDtypeStruct((H, entries), F32),
    )
    return stage_call(finish_kernel, outs, own, table, *gots, w_qkv, gain)


def flat_permute(value, mask):
    total = lax.axis_size("lon") * lax.axis_size("lat")
    return lax.ppermute(value, ("lon", "lat"), [(n, n ^ mask) for n in range(total)])


def bit_groups(total):
    bits = total.bit_length() - 1
    sizes = [1]
    while sum(sizes) < bits:
        sizes.append(min(2, bits - sum(sizes)))
    return sizes


def scatter_sum(matrix):
    n_lat = lax.axis_size("lat")
    total = lax.axis_size("lon") * n_lat
    me = lax.axis_index("lon") * n_lat + lax.axis_index("lat")
    rows, cols = matrix.shape
    blocks = matrix.reshape(total, rows // total, cols)
    low = 0
    sizes = bit_groups(total)
    for size in sizes:
        ways = 1 << size
        mine = (me >> low) & (ways - 1)
        view = blocks.reshape(blocks.shape[0] // ways, ways, rows // total, cols)
        kept = lax.dynamic_index_in_dim(view, mine, 1, keepdims=False).astype(F32)
        for n in range(1, ways):
            sent = lax.dynamic_index_in_dim(view, mine ^ n, 1, keepdims=False)
            kept = kept + flat_permute(sent, n << low).astype(F32)
        low += size
        blocks = kept if low == sum(sizes) else kept.astype(BF)
    return blocks.reshape(rows // total, cols)


def full_sum(value):
    total = lax.axis_size("lon") * lax.axis_size("lat")
    low = 0
    for size in bit_groups(total):
        value = pair_sum(value, [flat_permute(value, n << low) for n in range(1, 1 << size)])
        low += size
    return value


def ring_shift(value, steps):
    count = lax.axis_size("lon")
    return lax.ppermute(value, "lon", [(n, (n + steps) % count) for n in range(count)])


def step(inputs, d_out, w_qkv, w_proj, gain, bias_table, rel_index, shifts):
    n_lon = lax.axis_size("lon")
    n_lat = lax.axis_size("lat")
    n_dev = n_lon * n_lat
    _, columns, c = inputs.shape
    tokens = inputs.shape[0] * columns * n_dev
    scales = (tokens ** (-0.5), (tokens // WIN) ** (-0.5))
    entries = bias_table.shape[0]
    gain_row = gain.reshape(1, c)
    split = c // n_dev == UNIT and n_lat == 4

    *carried, w_qkv, w_proj, edge, last, hot, bias = before(
        shifts, rel_index, bias_table.T, gain_row, inputs, d_out, w_qkv, w_proj
    )
    halo = ring_shift(last, 1)
    early = attend_first(EARLY, carried[3], carried[4], bias)
    x, d, nt, qkv, dh = project_rim(shifts, halo, edge, w_qkv, w_proj, gain_row, early[2], carried)
    dp, *out = attend(qkv, dh, bias, hot, nt, d, early, scales, n_dev, split)
    if split:
        kept, sent, table = out
        got = flat_permute(sent, 1)
    first = input_rim(dp, x, d, w_qkv, gain_row)
    returned = ring_shift(first, -1)
    if split:
        own_a, sent_a, own_b, sent_b, table = core_stage(kept, got, table)
        got_a, got_b = flat_permute(sent_a, 2), flat_permute(sent_b, 4)
    grid, end = input_rest(shifts, dp, x, d, w_qkv, gain_row, first)
    if split:
        own_a, sent_a, own_b, sent_b, table = pair_stage(own_a, got_a, own_b, got_b, table)
        got_a, got_b = flat_permute(sent_a, 4), flat_permute(sent_b, 2)
    d_inputs = place_last(shifts, end, returned, grid)
    if split:
        own, *sent, table = top_stage(own_a, got_a, own_b, got_b, table)
        gots = [flat_permute(value, n << 3) for n, value in enumerate(sent, 1)]
        g_qkv, g_proj, g_gain, g_table = finish(own, table, gots, w_qkv, gain_row, entries)
        return (d_inputs, g_qkv, g_proj, g_gain.reshape(UNIT), g_table.T)

    own = scatter_sum(jnp.concatenate(out[:2], axis=1))
    g_qkv, g_proj = own[:, : 3 * c], own[:, 3 * c :]
    g_table = full_sum(out[2]).T
    rows = c // n_dev
    me = device_index()
    w_rows = lax.dynamic_slice_in_dim(w_qkv, me * rows, rows, 0).astype(F32)
    gain_rows = lax.dynamic_slice_in_dim(gain, me * rows, rows, 0)
    g_gain = jnp.sum(w_rows * g_qkv, axis=1) / gain_rows
    return (d_inputs, g_qkv, g_proj, g_gain, g_table)


def solution(mesh):
    return jax.shard_map(
        step,
        mesh=mesh,
        in_specs=(P("lat", "lon", None), P("lat", "lon", None), P(), P(), P(), P(), P(), P("lat")),
        out_specs=(
            P("lat", "lon", None),
            P(("lon", "lat"), None),
            P(("lon", "lat"), None),
            P(("lon", "lat")),
            P(),
        ),
        check_vma=False,
    )
```
